32 devices in a mesh: gx: 4 (over z), gy: 8 (over y, x, core).
Axes of the slice: x: 2, y: 2, z: 4, core: 2. Of those that a mesh axis runs over, the one named last changes fastest.
Arguments:
- rhs: float32 [4, 8, 1, 3, 200, 128], P('gx', 'gy'), may hold values from -25 to 25
- stiff_inverse: bfloat16 [4, 8, 1, 1200, 1200], P('gx', 'gy'), may hold values from -2 to 6, as said below
- schur: bfloat16 [4, 8, 1, 1200, 1200], P('gx', 'gy'), may hold values from -2 to 6, as said below
- phi: bfloat16 [4, 8, 1, 24, 1200], P('gx', 'gy'), may hold values from -0.1875 to 0.1875
- coarse_inverse: float32 [192, 192], P(('gx', 'gy')), may hold values from -2 to 6, as said below
- incidence: int32 [4, 8, 1, 8], P('gx', 'gy'), may hold values from 0 to 63, as said below
- pairing: int32 [4, 8, 1, 3, 200], P('gx', 'gy'), may hold values from 0 to 199, as said below
Outputs:
- multipliers: float32 [4, 8, 1, 3, 200, 128], P('gx', 'gy')
- reduction: float32 [128], replicated
The draws below stay inside these ranges and needn't reach their ends.
Inputs may be any that keep to these rules, and one draw needn't show every extreme that they name: `stiff_inverse`: each block is symmetric positive definite. `schur`: each block is symmetric positive definite. `coarse_inverse`: symmetric positive definite. `incidence`: the corners of the subdomain grid, periodic in the first two dimensions, under an arbitrary numbering of the 64 nodes: corner c of subdomain (x, y, z) is the grid point (x + c % 2, y + (c // 2) % 2, z + c // 4), and subdomains that share a grid point name the same node. `pairing`: each row over the last dimension is a permutation of 0 to 199.
All inputs are finite; a program needn't handle non-finite values.
Results may differ from the reference program's by a relative error of at most 0.0027.
Values sent between devices are 32-bit elements; how exact they have to be, the bound alone decides.
A program may use at most 64 MiB of HBM per device.

```python
import math
import jax
import jax.numpy as jnp
from jax import lax

ORDER = 1200
FACE = 200
CORNER = 24
LOADS = 128
SUB_DEV = 1
ITERS = 2
GRID_X = 4
GRID_Y = 8
NODES = 64
COARSE = 192


def definite_block(key, size):
    noise = jax.random.normal(jax.random.fold_in(key, 1), (size, size), jnp.float32)
    coupled = (noise + noise.T) * (0.35 / math.sqrt(2.0 * size))
    diagonal = jax.random.uniform(jax.random.fold_in(key, 2), (size,), jnp.float32, 1.0, 2.0)
    block = coupled + jnp.diag(diagonal)
    return block


def block_stack(key):
    count = GRID_X * GRID_Y * SUB_DEV
    blocks = lax.map(lambda index: definite_block(jax.random.fold_in(key, index), ORDER).astype(jnp.bfloat16), jnp.arange(count))
    return blocks.reshape(GRID_X, GRID_Y, SUB_DEV, ORDER, ORDER)


def draw_stiff_inverse(key, part):
    return block_stack(jax.random.fold_in(key, 11))


def draw_schur(key, part):
    return block_stack(jax.random.fold_in(key, 23))


def draw_coarse_inverse(key, part):
    return definite_block(jax.random.fold_in(key, 37), COARSE)


def draw_rhs(key, part):
    count = GRID_X * GRID_Y * SUB_DEV
    shape = (GRID_X, GRID_Y, SUB_DEV, 3, FACE, LOADS)
    ramp = (jnp.arange(count, dtype=jnp.float32) / max(count - 1, 1)).reshape(GRID_X, GRID_Y, SUB_DEV, 1, 1, 1)
    scale = jnp.exp(math.log(3.0) * ramp)
    base = jax.random.truncated_normal(jax.random.fold_in(key, 63), -4.0, 4.0, shape, jnp.float32)
    return base * scale


def draw_incidence(key, part):
    dof_numbering = jax.random.permutation(jax.random.fold_in(key, 41), NODES).astype(jnp.int32)
    corner = jnp.arange(8, dtype=jnp.int32)
    first = jnp.arange(GRID_X, dtype=jnp.int32)[:, None, None, None] + corner % 2
    second = jnp.arange(GRID_Y, dtype=jnp.int32)[None, :, None, None] + corner // 2 % 2
    third = jnp.arange(SUB_DEV, dtype=jnp.int32)[None, None, :, None] + corner // 4
    node = (first % GRID_X * GRID_Y + second % GRID_Y) * (SUB_DEV + 1) + third
    return dof_numbering[node].astype(jnp.int32)


def draw_pairing(key, part):
    count = GRID_X * GRID_Y * SUB_DEV * 3
    subkeys = jax.random.split(jax.random.fold_in(key, 53), count)
    orderings = jax.vmap(lambda subkey: jax.random.permutation(subkey, FACE))(subkeys).astype(jnp.int32)
    return orderings.reshape(GRID_X, GRID_Y, SUB_DEV, 3, FACE)


def shard_levels(key, extent, pieces, low, high):
    def one(dim, blocks):
        draws = jax.random.uniform(jax.random.fold_in(jax.random.fold_in(key, 6), dim), (blocks,), jnp.float32, low / len(pieces), high / len(pieces))
        return jnp.repeat(jnp.exp(draws), extent[dim] // blocks).reshape((-1,) + (1,) * (len(extent) - dim - 1))

    loudness = one(*pieces[0])
    for cut in pieces[1:]:
        loudness = loudness * one(*cut)
    return loudness


def bell_draw(stream_key, dims, width, limit, pieces=(), held_as=jnp.bfloat16):
    values = jax.random.normal(stream_key, dims, jnp.float32) * width
    if len(pieces) > 0:
        values = shard_levels(stream_key, dims, pieces, -0.22, 0.18) * values
    return jnp.clip(values, min=-limit, max=limit).astype(held_as)


def setup_inputs(seed: int = 0) -> dict:
    key_list = jax.random.split(jax.random.key(seed), 8)
    rhs = draw_rhs(jax.random.fold_in(key_list[7], 71), 0)
    stiff_inverse = draw_stiff_inverse(jax.random.fold_in(key_list[7], 71), 0)
    schur = draw_schur(jax.random.fold_in(key_list[7], 71), 0)
    phi = bell_draw(key_list[3], (GRID_X, GRID_Y, SUB_DEV, CORNER, ORDER), ORDER ** -0.5, 0.1875, ((0, 4), (1, 8)))
    coarse_inverse = draw_coarse_inverse(jax.random.fold_in(key_list[7], 71), 0)
    incidence = draw_incidence(jax.random.fold_in(key_list[7], 71), 0)
    pairing = draw_pairing(jax.random.fold_in(key_list[7], 71), 0)
    return dict(rhs=rhs, stiff_inverse=stiff_inverse, schur=schur, phi=phi, coarse_inverse=coarse_inverse, incidence=incidence, pairing=pairing)


def reference(rhs, stiff_inverse, schur, phi, coarse_inverse, incidence, pairing):
    largest_index = lax.Precision.HIGHEST
    level = jnp.arange(SUB_DEV)[:, None]
    axis_id = jnp.arange(3)[None, :]
    active = jnp.where((level == SUB_DEV - 1) & (axis_id == 2), 0.0, 1.0)
    active = active.astype(jnp.float32)[None, None, :, :, None, None]
    inverse_pairing = jnp.argsort(pairing, axis=-1).astype(jnp.int32)
    coupling_matrix = phi.astype(jnp.float32)
    flat_ids = incidence.reshape(-1).astype(jnp.int32)

    def transpose_jump(values):
        masked = values * active
        moved = jnp.take_along_axis(masked, inverse_pairing[..., None], axis=4)
        lower_x = jnp.roll(moved[:, :, :, 0], 1, axis=0)
        lower_y = jnp.roll(moved[:, :, :, 1], 1, axis=1)
        lower_z = jnp.concatenate([jnp.zeros_like(moved[:, :, :1, 2]), moved[:, :, :-1, 2]], axis=2)
        return jnp.stack([-lower_x, masked[:, :, :, 0], -lower_y, masked[:, :, :, 1], -lower_z, masked[:, :, :, 2]], axis=3)

    def jump_field(field):
        upper_x = jnp.roll(field[:, :, :, 0], -1, axis=0)
        upper_y = jnp.roll(field[:, :, :, 2], -1, axis=1)
        upper_z = jnp.concatenate([field[:, :, 1:, 4], jnp.zeros_like(field[:, :, :1, 4])], axis=2)
        neighbour = jnp.stack([upper_x, upper_y, upper_z], axis=3)
        paired = jnp.take_along_axis(neighbour, pairing[..., None], axis=4)
        higher = jnp.stack([field[:, :, :, 1], field[:, :, :, 3], field[:, :, :, 5]], axis=3)
        return (higher - paired) * active

    def apply_local(matrices, field):
        flat_matrices = matrices.reshape(-1, ORDER, ORDER)
        flat_field = field.reshape(-1, ORDER, LOADS).astype(jnp.bfloat16)
        result = lax.map(lambda both: jnp.dot(both[0], both[1], preferred_element_type=jnp.float32), (flat_matrices, flat_field))
        return result.reshape(GRID_X, GRID_Y, SUB_DEV, 6, FACE, LOADS)

    def operator(values):
        field = transpose_jump(values)
        corner_load = jnp.einsum('xyzco,xyzor->xyzcr', coupling_matrix, field.reshape(GRID_X, GRID_Y, SUB_DEV, ORDER, LOADS), precision=largest_index)
        coarse_load = jax.ops.segment_sum(corner_load.reshape(-1, 3, LOADS), flat_ids, num_segments=NODES).reshape(COARSE, LOADS)
        coarse_solution = jnp.dot(coarse_inverse, coarse_load, precision=largest_index)
        corner_values = coarse_solution.reshape(NODES, 3, LOADS)[flat_ids].reshape(GRID_X, GRID_Y, SUB_DEV, CORNER, LOADS)
        spread_operator = jnp.einsum('xyzco,xyzcr->xyzor', coupling_matrix, corner_values, precision=largest_index)
        displacement = apply_local(stiff_inverse, field) + spread_operator.reshape(GRID_X, GRID_Y, SUB_DEV, 6, FACE, LOADS)
        return jump_field(displacement)

    def precondition(values):
        field = 0.5 * transpose_jump(values)
        return 0.5 * jump_field(apply_local(schur, field))

    def inner_product(left, right):
        return jnp.sum(left * right, axis=(0, 1, 2, 3, 4))

    residual = rhs * active
    multipliers = jnp.zeros_like(residual)
    preconditioned = precondition(residual)
    energy = inner_product(residual, preconditioned)
    start_energy = energy
    direction = preconditioned
    for iteration in range(ITERS):
        product_field = operator(direction)
        alpha = energy / inner_product(direction, product_field)
        multipliers = multipliers + alpha * direction
        residual = residual - alpha * product_field
        preconditioned = precondition(residual)
        energy_next = inner_product(residual, preconditioned)
        if iteration + 1 < ITERS:
            direction = preconditioned + (energy_next / energy) * direction
        energy = energy_next
    return multipliers, energy / start_energy
```

```python
import functools

import jax
import jax.numpy as jnp
from jax import lax
from jax.experimental import pallas as pl
from jax.experimental.pallas import tpu as pltpu
from jax.sharding import PartitionSpec as P

ITERS = 2
EXCHANGES = 2 * ITERS
SUMS = 2 * ITERS + 1
MESH = pl.DeviceIdType.MESH
F32 = jnp.float32
BF16 = jnp.bfloat16


def split(value, parts):
    pieces = []
    for _ in range(parts):
        piece = value.astype(BF16)
        pieces.append(piece)
        value = value - piece.astype(F32)
    return pieces


def narrow_dot(matrix, value, parts):
    width = value.shape[1]
    product = jnp.dot(
        matrix, jnp.concatenate(split(value, parts), axis=1), preferred_element_type=F32
    )
    total = product[:, (parts - 1) * width :]
    for part in range(parts - 2, -1, -1):
        total = total + product[:, part * width : (part + 1) * width]
    return total


def window(face, faces):
    start = face * faces // 128 * 128
    offset = face * faces - start
    return start, offset, -(-(offset + faces) // 128) * 128


def square_window(face, faces):
    start = face * faces // 128 * 128
    offset = face * faces - start
    return start, offset, -(-(offset + faces) // 256) * 256


def kernel(
    nx, ny, rhs_hbm, stiff_hbm, schur_hbm, phi_ref, cinv_ref, inc_ref, pair_ref,
    mult_hbm, reduction_ref,
    rhs_v, stiff, schur, phi_f, spread, spread_t, near_phi, got_rhs, got_pair, got,
    field, way, image, sums_out, sums_in, ids_out, ids_in, cinv_out, cinv_in, middle, inverse,
    part_out, part_in, part_own, load_x, load_y, loads_v, solved, lift, mult_v,
    local_sem, setup_send, setup_recv, face_send, face_recv, sum_send, sum_recv,
    all_send, all_recv, part_send, part_recv, load_send, load_recv,
):
    n = nx * ny
    faces = rhs_v.shape[1]
    cases = rhs_v.shape[2]
    jumps = 4 * faces
    coarse = cinv_in.shape[3]
    slots = n * 8
    ix, iy = lax.axis_index("gx"), lax.axis_index("gy")
    me = ix * ny + iy

    def at(dx, dy):
        return lax.rem(ix + (dx + nx), nx), lax.rem(iy + (dy + ny), ny)

    across = [at(-1, 0), at(1, 0), at(0, -1), at(0, 1)]
    rows = [pl.ds(f * faces, faces) for f in range(6)]

    loads = [
        pltpu.make_async_copy(rhs_hbm, rhs_v, local_sem.at[0]),
        pltpu.make_async_copy(schur_hbm, schur, local_sem.at[1]),
        pltpu.make_async_copy(stiff_hbm, stiff, local_sem.at[2]),
    ]
    for copy in loads:
        copy.start()

    ways_x = [at(d, 0)[0] for d in range(nx)]
    ways_y = [at(0, d)[1] for d in range(ny)]
    peers_x = [(x, iy) for x in ways_x[1:]]
    peers_y = [(ix, y) for y in ways_y[1:]]

    def each_peer(act):
        if n <= 64:
            for x in range(nx):
                for y in range(ny):
                    if x or y:
                        act((ways_x[x], ways_y[y]))
            return

        def step(k, carry):
            other = lax.rem(me + k, n)
            act((lax.div(other, ny), lax.rem(other, ny)))
            return carry

        lax.fori_loop(1, n, step, 0)

    barrier = pltpu.get_barrier_semaphore()
    each_peer(lambda target: pl.semaphore_signal(
        barrier, inc=1, device_id=target, device_id_type=MESH))

    corners = phi_ref.shape[0]
    row = lax.broadcasted_iota(jnp.int32, (32, corners), 0)
    col = lax.broadcasted_iota(jnp.int32, (32, corners), 1)
    point, inner = lax.div(row, 8), lax.rem(row, 8)
    source = 3 * (point + 4 * lax.div(inner, 3)) + lax.rem(inner, 3)
    order = jnp.where((col == source) & (inner < 6), 1.0, 0.0)
    phi_f[...] = jnp.dot(order.astype(BF16), phi_ref[...], preferred_element_type=F32)
    row = lax.broadcasted_iota(jnp.int32, (8, 8), 0)
    col = lax.broadcasted_iota(jnp.int32, (8, 8), 1)
    ids = jnp.broadcast_to(inc_ref[...].astype(F32), (8, 8))
    ids = jnp.sum(jnp.where(col == 4 * lax.div(row, 3), ids, 0.0), axis=1, keepdims=True)
    row = lax.broadcasted_iota(jnp.int32, ids_out.shape, 0)
    ids = 3.0 * jnp.broadcast_to(ids, ids_out.shape) + lax.rem(row, 3).astype(F32)
    ids = jnp.where(row < 6, ids, -1.0)
    ids_out[...] = ids
    ids_in[iy, ix] = ids
    own = jnp.concatenate([cinv_ref[...], jnp.zeros((2, coarse), F32)], axis=0)
    cinv_out[...] = own
    cinv_in[iy, ix] = own

    loads[0].wait()
    pl.semaphore_wait(barrier, n - 1)

    def send(src, dst, send_sem, recv_sem, target):
        copy = pltpu.make_async_remote_copy(
            src_ref=src, dst_ref=dst, send_sem=send_sem, recv_sem=recv_sem,
            device_id=target, device_id_type=MESH,
        )
        copy.start()
        return copy

    def to_all(src, slots, send_sem, recv_sem):
        each_peer(lambda target: send(src, slots.at[me], send_sem, recv_sem, target))

    def to_line(src, dst, send_sem, recv_sem, targets):
        for target in targets:
            send(src, dst, send_sem, recv_sem, target)

    def wait_all(slots, sem):
        whole = slots.at[pl.ds(0, slots.shape[0] - 1)]
        pltpu.make_async_copy(whole, whole, sem).wait()

    setup = []
    for a in range(2):
        setup.append(send(pair_ref.at[a], got_pair.at[a], setup_send.at[a], setup_recv.at[a],
                          across[2 * a + 1]))
    for a in range(2):
        setup.append(send(rhs_v.at[a], got_rhs.at[a], setup_send.at[2 + a],
                          setup_recv.at[2 + a], across[2 * a + 1]))
    for f in range(4):
        start, _, width = window(f, faces)
        partner = f ^ 1
        setup.append(send(phi_f.at[:, pl.ds(start, width)],
                          near_phi.at[partner, :, pl.ds(0, width)],
                          setup_send.at[4 + f], setup_recv.at[4 + partner], across[f]))
    to_line(ids_out, ids_in.at[iy, ix], all_send.at[0], all_recv.at[0], peers_x)
    to_line(cinv_out, cinv_in.at[iy, ix], all_send.at[1], all_recv.at[1], peers_x)

    def turned(pair_row, offset, width):
        lanes = lax.broadcasted_iota(jnp.int32, (1, width), 1)
        if width > faces:
            pair_row = jnp.concatenate(
                [pair_row, jnp.zeros((1, width - faces), jnp.int32)], axis=1
            )
        if offset:
            pair_row = pltpu.roll(pair_row, offset, axis=1)
        inside = (lanes >= offset) & (lanes < offset + faces)
        target = jnp.where(inside, pair_row + offset, lanes)
        place = lax.broadcasted_iota(jnp.int32, (width, width), 0)
        return jnp.where(place == target, 1.0, 0.0)

    turns = []
    for a in range(2):
        setup[a].wait_recv()
        start, offset, width = square_window(2 * a, faces)
        by_col = turned(got_pair[a], offset, width)
        turns.append((start, width, by_col.T.astype(BF16), by_col.astype(BF16)))

    def reorder(matrix):
        for start, width, by_row, _ in turns:
            band = matrix[pl.ds(start, width), :]
            matrix[pl.ds(start, width), :] = jnp.dot(
                by_row, band, preferred_element_type=F32
            ).astype(BF16)
        for start, width, _, by_col in turns:
            band = matrix[:, pl.ds(start, width)]
            matrix[:, pl.ds(start, width)] = jnp.dot(
                band, by_col, preferred_element_type=F32
            ).astype(BF16)

    loads[1].wait()
    reorder(schur)

    spread[pl.ds(0, 32), :] = phi_f[:, pl.ds(0, spread.shape[1])].astype(BF16)
    for start, width, _, by_col in turns:
        spread[pl.ds(0, 32), pl.ds(start, width)] = jnp.dot(
            spread[pl.ds(0, 32), pl.ds(start, width)], by_col, preferred_element_type=F32
        ).astype(BF16)
    spread[pl.ds(32, 128), :] = jnp.zeros((128, spread.shape[1]), BF16)

    def apply_local(matrix, low, k):
        sent = []
        for half in range(3):
            part = pl.ds(2 * half * faces, 2 * faces)
            image[k, part, :] = jnp.dot(matrix[part, :], low, preferred_element_type=F32)
            if half < 2:
                for f in (2 * half, 2 * half + 1):
                    sent.append(send(image.at[k, rows[f]], got.at[k, f ^ 1],
                                     face_send.at[k, f], face_recv.at[k, f ^ 1], across[f]))
        return sent

    def start_sum(partial, k):
        total = jnp.sum(partial, axis=0, keepdims=True)
        sums_out[k] = total
        sums_in[k, me] = total
        to_all(sums_out.at[k], sums_in.at[k], sum_send.at[k], sum_recv.at[k])

    def finish_sum(k):
        wait_all(sums_in.at[k], sum_recv.at[k])
        return jnp.sum(sums_in[k], axis=0)

    def wait_faces(k):
        for f in range(4):
            pltpu.make_async_copy(got.at[k, f], got.at[k, f], face_recv.at[k, f]).wait()

    zeros = jnp.zeros((2 * faces, cases), F32)
    for a in range(2):
        setup[2 + a].wait_recv()
        field[rows[2 * a], :] = -got_rhs[a]
        field[rows[2 * a + 1], :] = rhs_v[a]
    field[pl.ds(jumps, 2 * faces), :] = zeros
    for k in range(ITERS):
        way[k, pl.ds(jumps, 2 * faces), :] = zeros

    sent = []

    def precondition(k, s):
        half = 0.5 * field[...]
        sent.extend(apply_local(schur, half.astype(BF16), k))
        start_sum(half * image[k], s)

    def couple():
        for f in range(4):
            setup[4 + (f ^ 1)].wait_recv()
            start, offset, width = window(f, faces)
            _, other_offset, other_width = window(f ^ 1, faces)
            other = near_phi[f, :, pl.ds(0, other_width)]
            if f % 2:
                by_col = turned(pair_ref[f // 2], other_offset, other_width)
                other = jnp.dot(other.astype(BF16), by_col.astype(BF16),
                                preferred_element_type=F32)
            if other_width < width:
                other = jnp.concatenate(
                    [other, jnp.zeros((32, width - other_width), F32)], axis=1
                )
            both = other.shape[1]
            other = pltpu.roll(other, (offset - other_offset) % both, axis=1)
            lanes = lax.broadcasted_iota(jnp.int32, (32, both), 1)
            inside = (lanes >= offset) & (lanes < offset + faces)
            other = jnp.where(inside, -other, 0.0)[:, 0:width]
            spread[pl.ds(32 + 32 * f, 32), pl.ds(start, width)] = other.astype(BF16)

    def start_loads(k, it):
        value = narrow_dot(spread[:, pl.ds(0, jumps)], image[k, pl.ds(0, jumps), :], 2)

        def own(b, a):
            return 0.5 * value[8 * (2 * b + a) : 8 * (2 * b + a) + 8]

        def near(f, b, a):
            return 0.5 * value[32 + 32 * f + 8 * (2 * b + a) : 40 + 32 * f + 8 * (2 * b + a)]

        for b in range(2):
            line = jnp.concatenate([
                near(0, b, 0),
                own(b, 0) + near(0, b, 1) + near(2 + b, 1 - b, 0),
                own(b, 1) + near(1, b, 0) + near(2 + b, 1 - b, 1),
                near(1, b, 1),
            ], axis=0)
            if b:
                part_out[it, pl.ds(0, 32), :] = line
            else:
                part_own[it] = line
        part_out[it, pl.ds(32, 16), :] = jnp.concatenate([near(2, 0, 0), near(2, 0, 1)], axis=0)
        part_out[it, pl.ds(48, 16), :] = jnp.concatenate([near(3, 1, 0), near(3, 1, 1)], axis=0)
        for j, (start, size, dy) in enumerate(((0, 32, 1), (32, 16, -1), (48, 16, 2))):
            part = pl.ds(start, size)
            sent.append(send(part_out.at[it, part], part_in.at[it, part], part_send.at[it, j],
                             part_recv.at[it, j], at(0, dy)))

    def pass_loads(it):
        for j, (start, size) in enumerate(((0, 32), (32, 16), (48, 16))):
            part = part_in.at[it, pl.ds(start, size)]
            pltpu.make_async_copy(part, part, part_recv.at[it, j]).wait()
        line = part_own[it] + part_in[it, pl.ds(0, 32), :]
        inner = part_in[it, pl.ds(32, 16), :] + part_in[it, pl.ds(48, 16), :]
        edge = jnp.zeros((8, cases), F32)
        load_x[it, ix] = line + jnp.concatenate([edge, inner, edge], axis=0)
        to_line(load_x.at[it, ix], load_x.at[it, ix], load_send.at[it], load_recv.at[it],
                peers_x)

    def share_loads(it):
        wait_all(load_x.at[it], load_recv.at[it])
        for x in range(nx):
            total = load_x[it, (x + 1) % nx, pl.ds(0, 8), :]
            for a in range(3):
                total = total + load_x[it, (x - a) % nx, pl.ds(8 * a + 8, 8), :]
            load_y[it, iy, pl.ds(8 * x, 8), :] = total
        to_line(load_y.at[it, iy], load_y.at[it, iy], load_send.at[ITERS + it],
                load_recv.at[ITERS + it], peers_y)

    block = min(256, slots)
    blocks = slots // block

    def each_block(act):
        if blocks == 1:
            act(0)
            return

        def step(g, carry):
            act(pl.multiple_of(g * block, block))
            return carry

        lax.fori_loop(0, blocks, step, 0)

    def prepare_coarse():
        wait_all(ids_in, all_recv.at[2])
        wait_all(cinv_in, all_recv.at[3])
        per_y = nx * 8
        group = block // per_y

        def order_columns(part, start):
            first = start if isinstance(start, int) else lax.div(start, per_y)
            raw = cinv_in[pl.ds(first, group)].reshape(block, coarse)
            dofs = ids_in[...].reshape(slots, 128)[:, 0:1]
            spot = lax.broadcasted_iota(jnp.int32, (slots, coarse), 1).astype(F32)
            pick = jnp.where(spot == dofs, 1.0, 0.0).astype(BF16)
            middle[pl.ds(start, block), :] = lax.dot_general(
                split(raw, 2)[part], pick, (((1,), (1,)), ((), ())), preferred_element_type=F32
            ).astype(BF16)

        def order_rows(part, start):
            first = start if isinstance(start, int) else lax.div(start, per_y)
            dofs = ids_in[pl.ds(first, group)].reshape(block, 128)[:, 0:1]
            spot = lax.broadcasted_iota(jnp.int32, (block, slots), 1)
            device = lax.div(spot, 8)
            inner = lax.rem(spot, 8)
            device = lax.rem(device, nx) * ny + lax.div(device, nx)
            held = jnp.where(inner < 6, 6 * device + inner, -2).astype(F32)
            pick = jnp.where(held == dofs, 1.0, 0.0).astype(BF16)
            inverse[part, pl.ds(start, block), :] = jnp.dot(
                pick, middle[...], preferred_element_type=F32
            ).astype(BF16)

        for part in range(2):
            each_block(functools.partial(order_columns, part))
            each_block(functools.partial(order_rows, part))
        spread_t[...] = spread[:, pl.ds(0, jumps)].astype(F32).T.astype(BF16)

    def solve(it, ratio):
        wait_all(load_y.at[it], load_recv.at[ITERS + it])
        load = load_y[it].reshape(slots, cases)
        if it:
            load = load + ratio * loads_v[it - 1]
        loads_v[it] = load
        both = jnp.concatenate(split(load, 2), axis=1)

        def act(start):
            total = jnp.zeros((block, cases), F32)
            for part in (1, 0):
                product = jnp.dot(inverse[part, pl.ds(start, block), :], both,
                                  preferred_element_type=F32)
                total = total + product[:, cases:]
                total = total + product[:, 0:cases]
            first = start if isinstance(start, int) else lax.div(start, nx * 8)
            solved[pl.ds(first, block // (nx * 8))] = total.reshape(
                block // (nx * 8), nx, 8, cases)

        each_block(act)
        points = {}

        def point(dx, dy):
            if (dx, dy) not in points:
                x, y = at(dx, dy)
                points[dx, dy] = solved[y, x]
            return points[dx, dy]

        pieces = []
        for dx, dy in ((0, 0), (-1, 0), (1, 0), (0, -1), (0, 1)):
            pieces += [point(dx + a, dy + b) for b in range(2) for a in range(2)]
        lift[...] = narrow_dot(spread_t[...], jnp.concatenate(pieces, axis=0), 2)
        return jnp.sum(load * solved[...].reshape(slots, cases), axis=0, keepdims=True)

    precondition(0, 0)
    couple()
    energy = start_energy = None
    ratio = None
    alphas = []
    for it in range(ITERS):
        k = 2 * it
        start_loads(k, it)
        if it == 0:
            wait_all(ids_in.at[iy], all_recv.at[0])
            wait_all(cinv_in.at[iy], all_recv.at[1])
            to_line(ids_in.at[iy], ids_in.at[iy], all_send.at[2], all_recv.at[2], peers_y)
            to_line(cinv_in.at[iy], cinv_in.at[iy], all_send.at[3], all_recv.at[3], peers_y)
            loads[2].wait()
            reorder(stiff)
        pass_loads(it)
        if it:
            following = finish_sum(2 * it)
            ratio = following / energy
            energy = following
        wait_faces(k)
        for f in range(4):
            moved = 0.5 * (image[k, rows[f], :] - got[k, f])
            if it:
                moved = moved + ratio * way[it - 1, rows[f], :]
            way[it, rows[f], :] = moved
        walk = way[it]
        sent.extend(apply_local(stiff, walk.astype(BF16), k + 1))
        start_sum(walk * image[k + 1], 2 * it + 1)
        share_loads(it)
        if it == 0:
            prepare_coarse()
            energy = start_energy = finish_sum(0)
        coarse_part = solve(it, ratio)
        alpha = energy / (finish_sum(2 * it + 1) + coarse_part)
        alphas.append(alpha)
        wait_faces(k + 1)
        for f in range(4):
            jump = (image[k + 1, rows[f], :] - got[k + 1, f]) + lift[rows[f], :]
            field[rows[f], :] = field[rows[f], :] - alpha * jump
        if it + 1 < ITERS:
            precondition(k + 2, 2 * it + 2)
        else:
            half = 0.5 * field[...]
            product = jnp.dot(schur[...], half.astype(BF16), preferred_element_type=F32)
            start_sum(half * product, 2 * it + 2)

    for a in range(2):
        total = alphas[0] * way[0, rows[2 * a + 1], :]
        for it in range(1, ITERS):
            total = total + alphas[it] * way[it, rows[2 * a + 1], :]
        mult_v[a] = total
    mult_v[2] = jnp.zeros(mult_v.shape[1:], F32)
    result = pltpu.make_async_copy(mult_v, mult_hbm, local_sem.at[3])
    result.start()

    for copy in setup + sent:
        copy.wait_send()
    wait_all(ids_in.at[iy], all_send.at[0])
    wait_all(cinv_in.at[iy], all_send.at[1])
    wait_all(ids_in, all_send.at[2])
    wait_all(cinv_in, all_send.at[3])
    for it in range(ITERS):
        wait_all(load_x.at[it], load_send.at[it])
        wait_all(load_y.at[it], load_send.at[ITERS + it])
    for k in range(SUMS - 1):
        wait_all(sums_in.at[k], sum_send.at[k])
    result.wait()
    reduction_ref[...] = finish_sum(SUMS - 1) / start_energy
    wait_all(sums_in.at[SUMS - 1], sum_send.at[SUMS - 1])


def finish(mult_ref, reduction_ref, mult_out, reduction_out):
    mult_out[...] = mult_ref[...]
    reduction_out[...] = reduction_ref[...]


def local(nx, ny, rhs, stiff_inverse, schur, phi, coarse_inverse, incidence, pairing):
    n = nx * ny
    faces, cases = rhs.shape[4], rhs.shape[5]
    interface = stiff_inverse.shape[3]
    corners = phi.shape[3]
    coarse = coarse_inverse.shape[1]
    nodes = incidence.shape[3]
    slots = 8 * n
    wide = max(window(f, faces)[2] for f in range(4))
    reach = max(sum(window(f, faces)[::2]) for f in range(4))
    vmem = pl.BlockSpec(memory_space=pltpu.VMEM)
    anywhere = pl.BlockSpec(memory_space=pl.ANY)
    dma = pltpu.SemaphoreType.DMA
    shapes = (
        jax.ShapeDtypeStruct((3, faces, cases), F32),
        jax.ShapeDtypeStruct((1, cases), F32),
    )
    results = pl.pallas_call(
        functools.partial(kernel, nx, ny),
        out_shape=shapes,
        in_specs=[anywhere] * 3 + [vmem] * 4,
        out_specs=(anywhere, vmem),
        scratch_shapes=[
            pltpu.VMEM((3, faces, cases), F32),
            pltpu.VMEM((interface, interface), BF16),
            pltpu.VMEM((interface, interface), BF16),
            pltpu.VMEM((32, interface), F32),
            pltpu.VMEM((160, reach), BF16),
            pltpu.VMEM((4 * faces, 160), BF16),
            pltpu.VMEM((4, 32, wide), F32),
            pltpu.VMEM((2, faces, cases), F32),
            pltpu.VMEM((2, 1, faces), jnp.int32),
            pltpu.VMEM((EXCHANGES, 4, faces, cases), F32),
            pltpu.VMEM((interface, cases), F32),
            pltpu.VMEM((ITERS, interface, cases), F32),
            pltpu.VMEM((EXCHANGES, interface, cases), F32),
            pltpu.VMEM((SUMS, 1, cases), F32),
            pltpu.VMEM((SUMS, n, 1, cases), F32),
            pltpu.VMEM((8, 128), F32),
            pltpu.VMEM((ny, nx, 8, 128), F32),
            pltpu.VMEM((8, coarse), F32),
            pltpu.VMEM((ny, nx, 8, coarse), F32),
            pltpu.VMEM((slots, slots), BF16),
            pltpu.VMEM((2, slots, slots), BF16),
            pltpu.VMEM((ITERS, 64, cases), F32),
            pltpu.VMEM((ITERS, 64, cases), F32),
            pltpu.VMEM((ITERS, 32, cases), F32),
            pltpu.VMEM((ITERS, nx, 32, cases), F32),
            pltpu.VMEM((ITERS, ny, nx * 8, cases), F32),
            pltpu.VMEM((ITERS, slots, cases), F32),
            pltpu.VMEM((ny, nx, 8, cases), F32),
            pltpu.VMEM((4 * faces, cases), F32),
            pltpu.VMEM((3, faces, cases), F32),
            dma((4,)),
            dma((8,)),
            dma((8,)),
            dma((EXCHANGES, 4)),
            dma((EXCHANGES, 4)),
            dma((SUMS,)),
            dma((SUMS,)),
            dma((4,)),
            dma((4,)),
            dma((ITERS, 3)),
            dma((ITERS, 3)),
            dma((2 * ITERS,)),
            dma((2 * ITERS,)),
        ],
        compiler_params=pltpu.CompilerParams(
            collective_id=0, has_side_effects=True, vmem_limit_bytes=67043328
        ),
    )(
        rhs.reshape(3, faces, cases),
        stiff_inverse.reshape(interface, interface),
        schur.reshape(interface, interface),
        phi.reshape(corners, interface),
        coarse_inverse,
        incidence.reshape(1, nodes),
        pairing.reshape(3, 1, faces),
    )
    multipliers, reduction = pl.pallas_call(
        finish, out_shape=shapes, in_specs=[vmem] * 2, out_specs=(vmem, vmem)
    )(*results)
    return multipliers.reshape(rhs.shape), reduction.reshape(cases)


def solution(mesh):
    nx, ny = mesh.shape["gx"], mesh.shape["gy"]
    return jax.shard_map(
        functools.partial(local, nx, ny),
        mesh=mesh,
        in_specs=(
            P("gx", "gy", None, None, None, None),
            P("gx", "gy", None, None, None),
            P("gx", "gy", None, None, None),
            P("gx", "gy", None, None, None),
            P(("gx", "gy"), None),
            P("gx", "gy", None, None),
            P("gx", "gy", None, None, None),
        ),
        out_specs=(P("gx", "gy", None, None, None, None), P()),
        check_vma=False,
    )
```

```python
import functools

import jax
import jax.numpy as jnp
from jax import lax
from jax.experimental import pallas as pl
from jax.experimental.pallas import tpu as pltpu
from jax.sharding import PartitionSpec as P

ITERS = 2
EXCHANGES = 2 * ITERS
SUMS = 2 * ITERS + 1
SPLIT = (0, 1, 3)
MESH = pl.DeviceIdType.MESH
F32 = jnp.float32
BF16 = jnp.bfloat16


def split(value, parts):
    pieces = []
    for _ in range(parts):
        piece = value.astype(BF16)
        pieces.append(piece)
        value = value - piece.astype(F32)
    return pieces


def narrow_dot(matrix, value, parts):
    width = value.shape[1]
    product = jnp.dot(
        matrix, jnp.concatenate(split(value, parts), axis=1), preferred_element_type=F32
    )
    total = product[:, (parts - 1) * width :]
    for part in range(parts - 2, -1, -1):
        total = total + product[:, part * width : (part + 1) * width]
    return total


def window(face, faces):
    start = face * faces // 128 * 128
    offset = face * faces - start
    return start, offset, -(-(offset + faces) // 128) * 128


def square_window(face, faces):
    start = face * faces // 128 * 128
    offset = face * faces - start
    return start, offset, -(-(offset + faces) // 256) * 256


def kernel(
    nx, ny, rhs_hbm, stiff_hbm, schur_hbm, phi_hbm, cinv_hbm, inc_hbm, pair_hbm,
    mult_hbm, reduction_ref,
    rhs_v, stiff, schur, phi_ref, cinv_ref, inc_ref, pair_ref, phi_f, spread, spread_t, near_phi, got_rhs, got_pair, got,
    field, way, image, sums_out, sums_in, cinv_out, cinv_in, middle, inverse,
    part_out, part_in, part_own, load_x, load_y, loads_v, solved, lift, mult_v,
    local_sem, setup_send, setup_recv, face_send, face_recv, sum_send, sum_recv,
    all_send, all_recv, part_send, part_recv, load_send, load_recv,
):
    n = nx * ny
    faces = rhs_v.shape[1]
    interface = stiff.shape[0]
    cases = rhs_v.shape[2]
    jumps = 4 * faces
    coarse = cinv_hbm.shape[1]
    slots = n * 8
    span = phi_f.shape[2]
    ix, iy = lax.axis_index("gx"), lax.axis_index("gy")
    me = ix * ny + iy

    def at(dx, dy):
        return lax.rem(ix + (dx + nx), nx), lax.rem(iy + (dy + ny), ny)

    across = [at(-1, 0), at(1, 0), at(0, -1), at(0, 1)]
    rows = [pl.ds(f * faces, faces) for f in range(6)]

    sources = [rhs_hbm, pair_hbm, phi_hbm, inc_hbm, cinv_hbm, schur_hbm, stiff_hbm]
    targets = [rhs_v, pair_ref, phi_ref, inc_ref, cinv_ref, schur, stiff]
    loads = [
        pltpu.make_async_copy(source, target, local_sem.at[i])
        for i, (source, target) in enumerate(zip(sources, targets))
    ]

    ways_x = [at(d, 0)[0] for d in range(nx)]
    ways_y = [at(0, d)[1] for d in range(ny)]
    peers_x = [(x, iy) for x in ways_x[1:]]
    peers_y = [(ix, y) for y in ways_y[1:]]

    def each_peer(act):
        if n <= 64:
            for x in range(nx):
                for y in range(ny):
                    if x or y:
                        act((ways_x[x], ways_y[y]))
            return

        def step(k, carry):
            other = lax.rem(me + k, n)
            act((lax.div(other, ny), lax.rem(other, ny)))
            return carry

        lax.fori_loop(1, n, step, 0)

    for copy in loads[:5]:
        copy.start()
    barrier = pltpu.get_barrier_semaphore()
    each_peer(lambda target: pl.semaphore_signal(
        barrier, inc=1, device_id=target, device_id_type=MESH))

    for copy in loads[5:]:
        copy.start()

    corners = phi_ref.shape[0]
    row = lax.broadcasted_iota(jnp.int32, (32, corners), 0)
    col = lax.broadcasted_iota(jnp.int32, (32, corners), 1)
    point, inner = lax.div(row, 8), lax.rem(row, 8)
    source = 3 * (point + 4 * lax.div(inner, 3)) + lax.rem(inner, 3)
    order = jnp.where((col == source) & (inner < 6), 1.0, 0.0).astype(BF16)
    for i in range(1, 5):
        loads[i].wait()
    reach = spread.shape[1]
    whole_phi = phi_ref[:, pl.ds(0, reach)]
    spread[pl.ds(0, 32), :] = jnp.dot(
        order, whole_phi, preferred_element_type=F32
    ).astype(BF16)
    for f in range(4):
        start, offset, width = window(f, faces)
        piece = phi_ref[:, pl.ds(start, width)].astype(F32)
        if offset:
            piece = pltpu.roll(piece, width - offset, axis=1)
        phi_f[f] = piece[:, 0:span]
    row = lax.broadcasted_iota(jnp.int32, (8, 8), 0)
    col = lax.broadcasted_iota(jnp.int32, (8, 8), 1)
    ids = jnp.broadcast_to(inc_ref[...].astype(F32), (8, 8))
    ids = jnp.sum(jnp.where(col == 4 * lax.div(row, 3), ids, 0.0), axis=1, keepdims=True)
    wide = cinv_out.shape[1]
    row = lax.broadcasted_iota(jnp.int32, (8, wide), 0)
    ids = 3.0 * jnp.broadcast_to(ids, (8, wide)) + lax.rem(row, 3).astype(F32)
    ids = jnp.where(row < 6, ids, -1.0)
    own = jnp.concatenate([cinv_ref[...], jnp.zeros((2, coarse), F32)], axis=0)
    own = jnp.concatenate([own, jnp.zeros((8, wide - coarse), F32)], axis=1)
    lanes = lax.broadcasted_iota(jnp.int32, (8, wide), 1)
    own = jnp.where(lanes == coarse, ids, own)
    cinv_out[...] = own
    cinv_in[iy, ix] = own

    loads[0].wait()
    pl.semaphore_wait(barrier, n - 1)

    def send(src, dst, send_sem, recv_sem, target):
        copy = pltpu.make_async_remote_copy(
            src_ref=src, dst_ref=dst, send_sem=send_sem, recv_sem=recv_sem,
            device_id=target, device_id_type=MESH,
        )
        copy.start()
        return copy

    def to_all(src, slots, send_sem, recv_sem):
        each_peer(lambda target: send(src, slots.at[me], send_sem, recv_sem, target))

    def to_line(src, dst, send_sem, recv_sem, targets):
        for target in targets:
            send(src, dst, send_sem, recv_sem, target)

    def wait_all(slots, sem):
        whole = slots.at[pl.ds(0, slots.shape[0] - 1)]
        pltpu.make_async_copy(whole, whole, sem).wait()

    setup = []
    for a in range(2):
        setup.append(send(pair_ref.at[a], got_pair.at[a], setup_send.at[a], setup_recv.at[a],
                          across[2 * a + 1]))
    for a in range(2):
        setup.append(send(rhs_v.at[a], got_rhs.at[a], setup_send.at[2 + a],
                          setup_recv.at[2 + a], across[2 * a + 1]))
    for f in range(4):
        setup.append(send(phi_f.at[f], near_phi.at[f ^ 1], setup_send.at[4 + f],
                          setup_recv.at[4 + (f ^ 1)], across[f]))
    to_line(cinv_out, cinv_in.at[iy, ix], all_send.at[0], all_recv.at[0], peers_x)

    def turned(pair_row, offset, width):
        lanes = lax.broadcasted_iota(jnp.int32, (1, width), 1)
        if width > faces:
            pair_row = jnp.concatenate(
                [pair_row, jnp.zeros((1, width - faces), jnp.int32)], axis=1
            )
        if offset:
            pair_row = pltpu.roll(pair_row, offset, axis=1)
        inside = (lanes >= offset) & (lanes < offset + faces)
        target = jnp.where(inside, pair_row + offset, lanes)
        place = lax.broadcasted_iota(jnp.int32, (width, width), 0)
        return jnp.where(place == target, 1.0, 0.0)

    turns = []
    for a in range(2):
        setup[a].wait_recv()
        start, offset, width = square_window(2 * a, faces)
        by_col = turned(got_pair[a], offset, width)
        turns.append((start, width, by_col.T.astype(BF16), by_col.astype(BF16)))

    def reorder(matrix):
        for start, width, by_row, _ in turns:
            band = matrix[pl.ds(start, width), :]
            matrix[pl.ds(start, width), :] = jnp.dot(
                by_row, band, preferred_element_type=F32
            ).astype(BF16)
        for start, width, _, by_col in turns:
            band = matrix[:, pl.ds(start, width)]
            matrix[:, pl.ds(start, width)] = jnp.dot(
                band, by_col, preferred_element_type=F32
            ).astype(BF16)

    loads[5].wait()
    reorder(schur)

    for start, width, _, by_col in turns:
        spread[pl.ds(0, 32), pl.ds(start, width)] = jnp.dot(
            spread[pl.ds(0, 32), pl.ds(start, width)], by_col, preferred_element_type=F32
        ).astype(BF16)
    spread[pl.ds(32, 128), :] = jnp.zeros((128, spread.shape[1]), BF16)

    cut = 2 * faces
    low_cut, high_cut = cut // 128 * 128, -(-cut // 128) * 128

    def multiply_y(matrix, value, k, part):
        low = value[cut:].astype(BF16)
        if cut > low_cut:
            low = jnp.concatenate([jnp.zeros((cut - low_cut, cases), BF16), low], axis=0)
        image[k, part, :] = jnp.dot(matrix[part, pl.ds(low_cut, interface - low_cut)], low,
                                    preferred_element_type=F32)

    def multiply_x(matrix, value, k, part):
        low = value[0:cut].astype(BF16)
        if high_cut > cut:
            low = jnp.concatenate([low, jnp.zeros((high_cut - cut, cases), BF16)], axis=0)
        image[k, part, :] = image[k, part, :] + jnp.dot(
            matrix[part, pl.ds(0, high_cut)], low, preferred_element_type=F32)

    def multiply(matrix, value, k, part):
        image[k, part, :] = jnp.dot(matrix[part, :], value.astype(BF16),
                                    preferred_element_type=F32)

    last_x = jnp.where(ix == nx - 1, 1, 0)

    def send_faces(k, pair):
        for f in pair:
            if f < 2:
                f = last_x if f == 0 else 1 - last_x
                part = pl.ds(pl.multiple_of(f * faces, 8), faces)
                target = lax.rem(ix + 2 * f - 1 + nx, nx)
                sent.append(send(image.at[k, part], got.at[k, 1 - f], face_send.at[k, f],
                                 face_recv.at[k, 1 - f], (target, iy)))
                continue
            sent.append(send(image.at[k, rows[f]], got.at[k, f ^ 1], face_send.at[k, f],
                             face_recv.at[k, f ^ 1], across[f]))

    used, masked = pl.ds(0, jumps), pl.ds(jumps, interface - jumps)

    def start_sum(partial, k):
        total = jnp.sum(partial, axis=0, keepdims=True)
        sums_out[k] = total
        sums_in[k, me] = total
        to_all(sums_out.at[k], sums_in.at[k], sum_send.at[k], sum_recv.at[k])

    def finish_sum(k):
        wait_all(sums_in.at[k], sum_recv.at[k])
        return jnp.sum(sums_in[k], axis=0)

    def wait_faces(k, pair):
        for f in pair:
            pltpu.make_async_copy(got.at[k, f], got.at[k, f], face_recv.at[k, f]).wait()

    zeros = jnp.zeros((2 * faces, cases), F32)
    field[pl.ds(jumps, 2 * faces), :] = zeros
    for k in range(ITERS):
        way[k, pl.ds(jumps, 2 * faces), :] = zeros
    sent = []

    def precondition(k, s, ready):
        ready(1)
        if k in SPLIT:
            multiply_y(schur, 0.5 * field[...], k, used)
        ready(0)
        half = 0.5 * field[...]
        if k in SPLIT:
            multiply_x(schur, half, k, used)
        else:
            multiply(schur, half, k, used)
        start_sum(half[0:jumps] * image[k, used, :], s)
        if k == EXCHANGES:
            return
        send_faces(k, (0, 1))
        if k == 0:
            couple()
        start_loads(k, k // 2)
        send_faces(k, (2, 3))
        multiply(schur, half, k, masked)

    def first(a):
        setup[2 + a].wait_recv()
        field[rows[2 * a], :] = -got_rhs[a]
        field[rows[2 * a + 1], :] = rhs_v[a]

    def couple():
        near = []
        for f in range(4):
            setup[4 + (f ^ 1)].wait_recv()
            other = near_phi[f].astype(BF16)
            if f % 2:
                by_col = turned(pair_ref[f // 2], 0, span).astype(BF16)
                other = jnp.dot(other, by_col, preferred_element_type=F32).astype(BF16)
            near.append(other)
        near = jnp.dot(order, jnp.concatenate(near, axis=1), preferred_element_type=F32)
        for f in range(4):
            start, offset, width = window(f, faces)
            other = near[:, f * span : (f + 1) * span]
            if span < width:
                other = jnp.concatenate([other, jnp.zeros((32, width - span), F32)], axis=1)
            if offset:
                other = pltpu.roll(other, offset, axis=1)
            lanes = lax.broadcasted_iota(jnp.int32, (32, width), 1)
            inside = (lanes >= offset) & (lanes < offset + faces)
            other = jnp.where(inside, -other, 0.0)
            spread[pl.ds(32 + 32 * f, 32), pl.ds(start, width)] = other.astype(BF16)

    def start_loads(k, it):
        value = narrow_dot(spread[:, pl.ds(0, jumps)], image[k, pl.ds(0, jumps), :], 2)

        def own(b, a):
            return 0.5 * value[8 * (2 * b + a) : 8 * (2 * b + a) + 8]

        def near(f, b, a):
            return 0.5 * value[32 + 32 * f + 8 * (2 * b + a) : 40 + 32 * f + 8 * (2 * b + a)]

        for b in range(2):
            line = jnp.concatenate([
                near(0, b, 0),
                own(b, 0) + near(0, b, 1) + near(2 + b, 1 - b, 0),
                own(b, 1) + near(1, b, 0) + near(2 + b, 1 - b, 1),
                near(1, b, 1),
            ], axis=0)
            if b:
                part_out[it, pl.ds(0, 32), :] = line
            else:
                part_own[it] = line
        part_out[it, pl.ds(32, 16), :] = jnp.concatenate([near(2, 0, 0), near(2, 0, 1)], axis=0)
        part_out[it, pl.ds(48, 16), :] = jnp.concatenate([near(3, 1, 0), near(3, 1, 1)], axis=0)
        for j, (start, size, dy) in enumerate(((0, 32, 1), (32, 16, -1), (48, 16, 2))):
            part = pl.ds(start, size)
            sent.append(send(part_out.at[it, part], part_in.at[it, part], part_send.at[it, j],
                             part_recv.at[it, j], at(0, dy)))

    def pass_loads(it):
        for j, (start, size) in enumerate(((0, 32), (32, 16), (48, 16))):
            part = part_in.at[it, pl.ds(start, size)]
            pltpu.make_async_copy(part, part, part_recv.at[it, j]).wait()
        line = part_own[it] + part_in[it, pl.ds(0, 32), :]
        inner = part_in[it, pl.ds(32, 16), :] + part_in[it, pl.ds(48, 16), :]
        edge = jnp.zeros((8, cases), F32)
        load_x[it, ix] = line + jnp.concatenate([edge, inner, edge], axis=0)
        to_line(load_x.at[it, ix], load_x.at[it, ix], load_send.at[it], load_recv.at[it],
                peers_x)

    def share_loads(it):
        wait_all(load_x.at[it], load_recv.at[it])
        for x in range(nx):
            total = load_x[it, (x + 1) % nx, pl.ds(0, 8), :]
            for a in range(3):
                total = total + load_x[it, (x - a) % nx, pl.ds(8 * a + 8, 8), :]
            load_y[it, iy, pl.ds(8 * x, 8), :] = total
        to_line(load_y.at[it, iy], load_y.at[it, iy], load_send.at[ITERS + it],
                load_recv.at[ITERS + it], peers_y)

    block = min(256, slots)
    blocks = slots // block

    def each_block(act):
        if blocks == 1:
            act(0)
            return

        def step(g, carry):
            act(pl.multiple_of(g * block, block))
            return carry

        lax.fori_loop(0, blocks, step, 0)

    def prepare_coarse():
        wait_all(cinv_in, all_recv.at[1])
        per_y = nx * 8
        group = block // per_y

        def order_columns(part, start):
            first = start if isinstance(start, int) else lax.div(start, per_y)
            raw = cinv_in[pl.ds(first, group)].reshape(block, wide)[:, 0:coarse]
            dofs = cinv_in[...].reshape(slots, wide)[:, coarse : coarse + 1]
            spot = lax.broadcasted_iota(jnp.int32, (slots, coarse), 1).astype(F32)
            pick = jnp.where(spot == dofs, 1.0, 0.0).astype(BF16)
            middle[pl.ds(start, block), :] = lax.dot_general(
                split(raw, 2)[part], pick, (((1,), (1,)), ((), ())), preferred_element_type=F32
            ).astype(BF16)

        def order_rows(part, start):
            first = start if isinstance(start, int) else lax.div(start, per_y)
            dofs = cinv_in[pl.ds(first, group)].reshape(block, wide)[:, coarse : coarse + 1]
            spot = lax.broadcasted_iota(jnp.int32, (block, slots), 1)
            device = lax.div(spot, 8)
            inner = lax.rem(spot, 8)
            device = lax.rem(device, nx) * ny + lax.div(device, nx)
            held = jnp.where(inner < 6, 6 * device + inner, -2).astype(F32)
            pick = jnp.where(held == dofs, 1.0, 0.0).astype(BF16)
            inverse[part, pl.ds(start, block), :] = jnp.dot(
                pick, middle[...], preferred_element_type=F32
            ).astype(BF16)

        for part in range(2):
            each_block(functools.partial(order_columns, part))
            each_block(functools.partial(order_rows, part))
        spread_t[...] = spread[:, pl.ds(0, jumps)].astype(F32).T.astype(BF16)

    def solve(it, ratio):
        wait_all(load_y.at[it], load_recv.at[ITERS + it])
        load = load_y[it].reshape(slots, cases)
        if it:
            load = load + ratio * loads_v[it - 1]
        loads_v[it] = load
        both = jnp.concatenate(split(load, 2), axis=1)

        def act(start):
            total = jnp.zeros((block, cases), F32)
            for part in (1, 0):
                product = jnp.dot(inverse[part, pl.ds(start, block), :], both,
                                  preferred_element_type=F32)
                total = total + product[:, cases:]
                total = total + product[:, 0:cases]
            first = start if isinstance(start, int) else lax.div(start, nx * 8)
            solved[pl.ds(first, block // (nx * 8))] = total.reshape(
                block // (nx * 8), nx, 8, cases)

        each_block(act)
        points = {}

        def point(dx, dy):
            if (dx, dy) not in points:
                x, y = at(dx, dy)
                points[dx, dy] = solved[y, x]
            return points[dx, dy]

        pieces = []
        for dx, dy in ((0, 0), (-1, 0), (1, 0), (0, -1), (0, 1)):
            pieces += [point(dx + a, dy + b) for b in range(2) for a in range(2)]
        lift[...] = narrow_dot(spread_t[...], jnp.concatenate(pieces, axis=0), 2)
        return jnp.sum(load * solved[...].reshape(slots, cases), axis=0, keepdims=True)

    precondition(0, 0, first)
    energy = start_energy = None
    ratio = None
    alphas = []
    for it in range(ITERS):
        k = 2 * it
        if it == 0:
            wait_all(cinv_in.at[iy], all_recv.at[0])
            to_line(cinv_in.at[iy], cinv_in.at[iy], all_send.at[1], all_recv.at[1], peers_y)
            loads[6].wait()
            reorder(stiff)
        pass_loads(it)
        if it:
            following = finish_sum(2 * it)
            ratio = following / energy
            energy = following
        for a in (1, 0):
            wait_faces(k, (2 * a, 2 * a + 1))
            for f in (2 * a, 2 * a + 1):
                moved = 0.5 * (image[k, rows[f], :] - got[k, f])
                if it:
                    moved = moved + ratio * way[it - 1, rows[f], :]
                way[it, rows[f], :] = moved
            if a and k + 1 in SPLIT:
                multiply_y(stiff, way[it], k + 1, used)
        walk = way[it]
        if k + 1 in SPLIT:
            multiply_x(stiff, walk, k + 1, used)
        else:
            multiply(stiff, walk, k + 1, used)
        start_sum(walk[0:jumps] * image[k + 1, used, :], 2 * it + 1)
        send_faces(k + 1, range(4))
        multiply(stiff, walk, k + 1, masked)
        share_loads(it)
        if it == 0:
            prepare_coarse()
            energy = start_energy = finish_sum(0)
        coarse_part = solve(it, ratio)
        alpha = energy / (finish_sum(2 * it + 1) + coarse_part)
        alphas.append(alpha)

        def moved_on(a, k=k + 1, alpha=alpha):
            wait_faces(k, (2 * a, 2 * a + 1))
            for f in (2 * a, 2 * a + 1):
                jump = (image[k, rows[f], :] - got[k, f]) + lift[rows[f], :]
                field[rows[f], :] = field[rows[f], :] - alpha * jump

        precondition(k + 2, 2 * it + 2, moved_on)

    for a in range(2):
        total = alphas[0] * way[0, rows[2 * a + 1], :]
        for it in range(1, ITERS):
            total = total + alphas[it] * way[it, rows[2 * a + 1], :]
        mult_v[a] = total
    mult_v[2] = jnp.zeros(mult_v.shape[1:], F32)
    result = pltpu.make_async_copy(mult_v, mult_hbm, local_sem.at[7])
    result.start()

    for copy in setup + sent:
        copy.wait_send()
    wait_all(cinv_in.at[iy], all_send.at[0])
    wait_all(cinv_in, all_send.at[1])
    for it in range(ITERS):
        wait_all(load_x.at[it], load_send.at[it])
        wait_all(load_y.at[it], load_send.at[ITERS + it])
    for k in range(SUMS - 1):
        wait_all(sums_in.at[k], sum_send.at[k])
    result.wait()
    reduction_ref[...] = finish_sum(SUMS - 1) / start_energy
    wait_all(sums_in.at[SUMS - 1], sum_send.at[SUMS - 1])


def finish(mult_ref, reduction_ref, mult_out, reduction_out):
    mult_out[...] = mult_ref[...]
    reduction_out[...] = reduction_ref[...]


def local(nx, ny, rhs, stiff_inverse, schur, phi, coarse_inverse, incidence, pairing):
    n = nx * ny
    faces, cases = rhs.shape[4], rhs.shape[5]
    interface = stiff_inverse.shape[3]
    corners = phi.shape[3]
    coarse = coarse_inverse.shape[1]
    nodes = incidence.shape[3]
    slots = 8 * n
    span = -(-faces // 128) * 128
    wide = (coarse // 128 + 1) * 128
    reach = max(sum(window(f, faces)[::2]) for f in range(4))
    vmem = pl.BlockSpec(memory_space=pltpu.VMEM)
    anywhere = pl.BlockSpec(memory_space=pl.ANY)
    dma = pltpu.SemaphoreType.DMA
    shapes = (
        jax.ShapeDtypeStruct((3, faces, cases), F32),
        jax.ShapeDtypeStruct((1, cases), F32),
    )
    results = pl.pallas_call(
        functools.partial(kernel, nx, ny),
        out_shape=shapes,
        in_specs=[anywhere] * 7,
        out_specs=(anywhere, vmem),
        scratch_shapes=[
            pltpu.VMEM((3, faces, cases), F32),
            pltpu.VMEM((interface, interface), BF16),
            pltpu.VMEM((interface, interface), BF16),
            pltpu.VMEM((corners, interface), BF16),
            pltpu.VMEM(coarse_inverse.shape, F32),
            pltpu.VMEM((1, nodes), jnp.int32),
            pltpu.VMEM((3, 1, faces), jnp.int32),
            pltpu.VMEM((4, corners, span), F32),
            pltpu.VMEM((160, reach), BF16),
            pltpu.VMEM((4 * faces, 160), BF16),
            pltpu.VMEM((4, corners, span), F32),
            pltpu.VMEM((2, faces, cases), F32),
            pltpu.VMEM((2, 1, faces), jnp.int32),
            pltpu.VMEM((EXCHANGES, 4, faces, cases), F32),
            pltpu.VMEM((interface, cases), F32),
            pltpu.VMEM((ITERS, interface, cases), F32),
            pltpu.VMEM((EXCHANGES + 1, interface, cases), F32),
            pltpu.VMEM((SUMS, 1, cases), F32),
            pltpu.VMEM((SUMS, n, 1, cases), F32),
            pltpu.VMEM((8, wide), F32),
            pltpu.VMEM((ny, nx, 8, wide), F32),
            pltpu.VMEM((slots, slots), BF16),
            pltpu.VMEM((2, slots, slots), BF16),
            pltpu.VMEM((ITERS, 64, cases), F32),
            pltpu.VMEM((ITERS, 64, cases), F32),
            pltpu.VMEM((ITERS, 32, cases), F32),
            pltpu.VMEM((ITERS, nx, 32, cases), F32),
            pltpu.VMEM((ITERS, ny, nx * 8, cases), F32),
            pltpu.VMEM((ITERS, slots, cases), F32),
            pltpu.VMEM((ny, nx, 8, cases), F32),
            pltpu.VMEM((4 * faces, cases), F32),
            pltpu.VMEM((3, faces, cases), F32),
            dma((8,)),
            dma((8,)),
            dma((8,)),
            dma((EXCHANGES, 4)),
            dma((EXCHANGES, 4)),
            dma((SUMS,)),
            dma((SUMS,)),
            dma((2,)),
            dma((2,)),
            dma((ITERS, 3)),
            dma((ITERS, 3)),
            dma((2 * ITERS,)),
            dma((2 * ITERS,)),
        ],
        compiler_params=pltpu.CompilerParams(
            collective_id=0, has_side_effects=True, vmem_limit_bytes=67043328
        ),
    )(
        rhs.reshape(3, faces, cases),
        stiff_inverse.reshape(interface, interface),
        schur.reshape(interface, interface),
        phi.reshape(corners, interface),
        coarse_inverse,
        incidence.reshape(1, nodes),
        pairing.reshape(3, 1, faces),
    )
    multipliers, reduction = pl.pallas_call(
        finish, out_shape=shapes, in_specs=[vmem] * 2, out_specs=(vmem, vmem)
    )(*results)
    return multipliers.reshape(rhs.shape), reduction.reshape(cases)


def solution(mesh):
    nx, ny = mesh.shape["gx"], mesh.shape["gy"]
    return jax.shard_map(
        functools.partial(local, nx, ny),
        mesh=mesh,
        in_specs=(
            P("gx", "gy", None, None, None, None),
            P("gx", "gy", None, None, None),
            P("gx", "gy", None, None, None),
            P("gx", "gy", None, None, None),
            P(("gx", "gy"), None),
            P("gx", "gy", None, None),
            P("gx", "gy", None, None, None),
        ),
        out_specs=(P("gx", "gy", None, None, None, None), P()),
        check_vma=False,
    )
```

```python
import functools

import jax
import jax.numpy as jnp
from jax import lax
from jax.experimental import pallas as pl
from jax.experimental.pallas import tpu as pltpu
from jax.sharding import PartitionSpec as P

ITERS = 2
EXCHANGES = 2 * ITERS
SUMS = 2 * ITERS + 1
SPLIT = (0, *range(1, EXCHANGES, 2))
MESH = pl.DeviceIdType.MESH
F32 = jnp.float32
BF16 = jnp.bfloat16


def split(value, parts):
    pieces = []
    for _ in range(parts):
        piece = value.astype(BF16)
        pieces.append(piece)
        value = value - piece.astype(F32)
    return pieces


def narrow_dot(matrix, value, parts):
    width = value.shape[1]
    product = jnp.dot(
        matrix, jnp.concatenate(split(value, parts), axis=1), preferred_element_type=F32
    )
    total = product[:, (parts - 1) * width :]
    for part in range(parts - 2, -1, -1):
        total = total + product[:, part * width : (part + 1) * width]
    return total


def window(face, faces):
    start = face * faces // 128 * 128
    offset = face * faces - start
    return start, offset, -(-(offset + faces) // 128) * 128


def square_window(face, faces):
    start = face * faces // 128 * 128
    offset = face * faces - start
    return start, offset, -(-(offset + faces) // 256) * 256


def kernel(
    nx, ny, rhs_hbm, stiff_hbm, schur_hbm, phi_hbm, cinv_hbm, inc_hbm, pair_hbm,
    mult_hbm, reduction_ref,
    rhs_v, stiff, schur, phi_ref, cinv_ref, inc_ref, pair_ref, phi_f, spread, spread_t, near_phi, got_rhs, got_pair, got,
    field, way, image, sums_out, sums_in, cinv_out, cinv_in, middle, inverse,
    part_out, part_in, part_own, load_x, load_y, loads_v, solved, lift, mult_v,
    local_sem, setup_send, setup_recv, face_send, face_recv, sum_send, sum_recv,
    all_send, all_recv, part_send, part_recv, load_send, load_recv,
):
    n = nx * ny
    faces = rhs_v.shape[1]
    interface = stiff.shape[0]
    cases = rhs_v.shape[2]
    jumps = 4 * faces
    coarse = cinv_hbm.shape[1]
    slots = n * 8
    span = phi_f.shape[2]
    ix, iy = lax.axis_index("gx"), lax.axis_index("gy")
    me = ix * ny + iy

    def at(dx, dy):
        return lax.rem(ix + (dx + nx), nx), lax.rem(iy + (dy + ny), ny)

    across = [at(-1, 0), at(1, 0), at(0, -1), at(0, 1)]
    rows = [pl.ds(f * faces, faces) for f in range(6)]

    sources = [rhs_hbm, pair_hbm, phi_hbm, inc_hbm, cinv_hbm, schur_hbm, stiff_hbm]
    targets = [rhs_v, pair_ref, phi_ref, inc_ref, cinv_ref, schur, stiff]
    loads = [
        pltpu.make_async_copy(source, target, local_sem.at[i])
        for i, (source, target) in enumerate(zip(sources, targets))
    ]

    ways_x = [at(d, 0)[0] for d in range(nx)]
    ways_y = [at(0, d)[1] for d in range(ny)]
    peers_x = [(x, iy) for x in ways_x[1:]]
    peers_y = [(ix, y) for y in ways_y[1:]]

    def each_peer(act):
        if n <= 64:
            for x in range(nx):
                for y in range(ny):
                    if x or y:
                        act((ways_x[x], ways_y[y]))
            return

        def step(k, carry):
            other = lax.rem(me + k, n)
            act((lax.div(other, ny), lax.rem(other, ny)))
            return carry

        lax.fori_loop(1, n, step, 0)

    for copy in loads[:5]:
        copy.start()
    barrier = pltpu.get_barrier_semaphore()
    each_peer(lambda target: pl.semaphore_signal(
        barrier, inc=1, device_id=target, device_id_type=MESH))

    for copy in loads[5:]:
        copy.start()

    corners = phi_ref.shape[0]
    row = lax.broadcasted_iota(jnp.int32, (32, corners), 0)
    col = lax.broadcasted_iota(jnp.int32, (32, corners), 1)
    point, inner = lax.div(row, 8), lax.rem(row, 8)
    source = 3 * (point + 4 * lax.div(inner, 3)) + lax.rem(inner, 3)
    order = jnp.where((col == source) & (inner < 6), 1.0, 0.0).astype(BF16)
    for i in range(1, 5):
        loads[i].wait()
    reach = spread.shape[1]
    whole_phi = phi_ref[:, pl.ds(0, reach)]
    spread[pl.ds(0, 32), :] = jnp.dot(
        order, whole_phi, preferred_element_type=F32
    ).astype(BF16)
    for f in range(4):
        start, offset, width = window(f, faces)
        piece = phi_ref[:, pl.ds(start, width)].astype(F32)
        if offset:
            piece = pltpu.roll(piece, width - offset, axis=1)
        phi_f[f] = piece[:, 0:span]
    row = lax.broadcasted_iota(jnp.int32, (8, 8), 0)
    col = lax.broadcasted_iota(jnp.int32, (8, 8), 1)
    ids = jnp.broadcast_to(inc_ref[...].astype(F32), (8, 8))
    ids = jnp.sum(jnp.where(col == 4 * lax.div(row, 3), ids, 0.0), axis=1, keepdims=True)
    wide = cinv_out.shape[1]
    row = lax.broadcasted_iota(jnp.int32, (8, wide), 0)
    ids = 3.0 * jnp.broadcast_to(ids, (8, wide)) + lax.rem(row, 3).astype(F32)
    ids = jnp.where(row < 6, ids, -1.0)
    own = jnp.concatenate([cinv_ref[...], jnp.zeros((2, coarse), F32)], axis=0)
    own = jnp.concatenate([own, jnp.zeros((8, wide - coarse), F32)], axis=1)
    lanes = lax.broadcasted_iota(jnp.int32, (8, wide), 1)
    own = jnp.where(lanes == coarse, ids, own)
    cinv_out[...] = own
    cinv_in[iy, ix] = own

    loads[0].wait()
    pl.semaphore_wait(barrier, n - 1)

    def send(src, dst, send_sem, recv_sem, target):
        copy = pltpu.make_async_remote_copy(
            src_ref=src, dst_ref=dst, send_sem=send_sem, recv_sem=recv_sem,
            device_id=target, device_id_type=MESH,
        )
        copy.start()
        return copy

    def to_all(src, slots, send_sem, recv_sem):
        each_peer(lambda target: send(src, slots.at[me], send_sem, recv_sem, target))

    def to_line(src, dst, send_sem, recv_sem, targets):
        for target in targets:
            send(src, dst, send_sem, recv_sem, target)

    def wait_all(slots, sem):
        whole = slots.at[pl.ds(0, slots.shape[0] - 1)]
        pltpu.make_async_copy(whole, whole, sem).wait()

    setup = []
    for a in range(2):
        setup.append(send(pair_ref.at[a], got_pair.at[a], setup_send.at[a], setup_recv.at[a],
                          across[2 * a + 1]))
    for a in range(2):
        setup.append(send(rhs_v.at[a], got_rhs.at[a], setup_send.at[2 + a],
                          setup_recv.at[2 + a], across[2 * a + 1]))
    for f in range(4):
        setup.append(send(phi_f.at[f], near_phi.at[f ^ 1], setup_send.at[4 + f],
                          setup_recv.at[4 + (f ^ 1)], across[f]))
    to_line(cinv_out, cinv_in.at[iy, ix], all_send.at[0], all_recv.at[0], peers_x)

    def turned(pair_row, offset, width):
        lanes = lax.broadcasted_iota(jnp.int32, (1, width), 1)
        if width > faces:
            pair_row = jnp.concatenate(
                [pair_row, jnp.zeros((1, width - faces), jnp.int32)], axis=1
            )
        if offset:
            pair_row = pltpu.roll(pair_row, offset, axis=1)
        inside = (lanes >= offset) & (lanes < offset + faces)
        target = jnp.where(inside, pair_row + offset, lanes)
        place = lax.broadcasted_iota(jnp.int32, (width, width), 0)
        return jnp.where(place == target, 1.0, 0.0)

    turns = []
    for a in range(2):
        setup[a].wait_recv()
        start, offset, width = square_window(2 * a, faces)
        by_col = turned(got_pair[a], offset, width)
        turns.append((start, width, by_col.T.astype(BF16), by_col.astype(BF16)))

    def reorder(matrix):
        for start, width, by_row, _ in turns:
            band = matrix[pl.ds(start, width), :]
            matrix[pl.ds(start, width), :] = jnp.dot(
                by_row, band, preferred_element_type=F32
            ).astype(BF16)
        for start, width, _, by_col in turns:
            band = matrix[:, pl.ds(start, width)]
            matrix[:, pl.ds(start, width)] = jnp.dot(
                band, by_col, preferred_element_type=F32
            ).astype(BF16)

    loads[5].wait()
    reorder(schur)

    for start, width, _, by_col in turns:
        spread[pl.ds(0, 32), pl.ds(start, width)] = jnp.dot(
            spread[pl.ds(0, 32), pl.ds(start, width)], by_col, preferred_element_type=F32
        ).astype(BF16)
    spread[pl.ds(32, 128), :] = jnp.zeros((128, spread.shape[1]), BF16)

    cut = 2 * faces
    ahead = faces // 32 * 8
    low_cut, high_cut = cut // 128 * 128, -(-cut // 128) * 128

    def multiply_y(matrix, value, k, part):
        low = value[cut:].astype(BF16)
        if cut > low_cut:
            low = jnp.concatenate([jnp.zeros((cut - low_cut, cases), BF16), low], axis=0)
        image[k, part, :] = jnp.dot(matrix[part, pl.ds(low_cut, interface - low_cut)], low,
                                    preferred_element_type=F32)

    def multiply_x(matrix, value, k, part):
        low = value[0:cut].astype(BF16)
        if high_cut > cut:
            low = jnp.concatenate([low, jnp.zeros((high_cut - cut, cases), BF16)], axis=0)
        image[k, part, :] = image[k, part, :] + jnp.dot(
            matrix[part, pl.ds(0, high_cut)], low, preferred_element_type=F32)

    def multiply(matrix, value, k, part):
        image[k, part, :] = jnp.dot(matrix[part, :], value.astype(BF16),
                                    preferred_element_type=F32)

    last_x = jnp.where(ix == nx - 1, 1, 0)

    def send_x(k, start, size):
        for f in (last_x, 1 - last_x):
            part = pl.ds(pl.multiple_of(f * faces + start, 8), size)
            target = lax.rem(ix + 2 * f - 1 + nx, nx)
            sent.append(send(image.at[k, part], got.at[k, 1 - f, pl.ds(start, size)],
                             face_send.at[k, f], face_recv.at[k, 1 - f], (target, iy)))

    def send_faces(k, pair):
        for f in pair:
            sent.append(send(image.at[k, rows[f]], got.at[k, f ^ 1], face_send.at[k, f],
                             face_recv.at[k, f ^ 1], across[f]))

    used, masked = pl.ds(0, jumps), pl.ds(jumps, interface - jumps)

    def start_sum(partial, k):
        total = jnp.sum(partial, axis=0, keepdims=True)
        sums_out[k] = total
        sums_in[k, me] = total
        to_all(sums_out.at[k], sums_in.at[k], sum_send.at[k], sum_recv.at[k])

    def finish_sum(k):
        wait_all(sums_in.at[k], sum_recv.at[k])
        return jnp.sum(sums_in[k], axis=0)

    def wait_faces(k, pair):
        for f in pair:
            pltpu.make_async_copy(got.at[k, f], got.at[k, f], face_recv.at[k, f]).wait()

    zeros = jnp.zeros((2 * faces, cases), F32)
    field[pl.ds(jumps, 2 * faces), :] = zeros
    for k in range(ITERS):
        way[k, pl.ds(jumps, 2 * faces), :] = zeros
    sent = []

    def precondition(k, s, ready):
        ready(1)
        if k in SPLIT:
            multiply_y(schur, 0.5 * field[...], k, used)
        ready(0)
        half = 0.5 * field[...]
        act = multiply_x if k in SPLIT else multiply
        act(schur, half, k, pl.ds(0, cut))
        if k == 0:
            send_x(k, 0, faces)
        elif k < EXCHANGES:
            send_x(k, 0, ahead)
        act(schur, half, k, pl.ds(cut, cut))
        if k:
            start_sum(half[0:jumps] * image[k, used, :], s)
        if k == EXCHANGES:
            return
        if k == 0:
            couple()
        else:
            send_x(k, ahead, faces - ahead)
        start_loads(k, k // 2)
        send_faces(k, (2, 3))
        if k == 0:
            start_sum(half[0:jumps] * image[k, used, :], s)
        multiply(schur, half, k, masked)

    def first(a):
        setup[2 + a].wait_recv()
        field[rows[2 * a], :] = -got_rhs[a]
        field[rows[2 * a + 1], :] = rhs_v[a]

    def couple():
        near = []
        for f in range(4):
            setup[4 + (f ^ 1)].wait_recv()
            other = near_phi[f].astype(BF16)
            if f % 2:
                by_col = turned(pair_ref[f // 2], 0, span).astype(BF16)
                other = jnp.dot(other, by_col, preferred_element_type=F32).astype(BF16)
            near.append(other)
        near = jnp.dot(order, jnp.concatenate(near, axis=1), preferred_element_type=F32)
        for f in range(4):
            start, offset, width = window(f, faces)
            other = near[:, f * span : (f + 1) * span]
            if span < width:
                other = jnp.concatenate([other, jnp.zeros((32, width - span), F32)], axis=1)
            if offset:
                other = pltpu.roll(other, offset, axis=1)
            lanes = lax.broadcasted_iota(jnp.int32, (32, width), 1)
            inside = (lanes >= offset) & (lanes < offset + faces)
            other = jnp.where(inside, -other, 0.0)
            spread[pl.ds(32 + 32 * f, 32), pl.ds(start, width)] = other.astype(BF16)

    def start_loads(k, it):
        value = narrow_dot(spread[:, pl.ds(0, jumps)], image[k, pl.ds(0, jumps), :], 2)

        def own(b, a):
            return 0.5 * value[8 * (2 * b + a) : 8 * (2 * b + a) + 8]

        def near(f, b, a):
            return 0.5 * value[32 + 32 * f + 8 * (2 * b + a) : 40 + 32 * f + 8 * (2 * b + a)]

        for b in range(2):
            line = jnp.concatenate([
                near(0, b, 0),
                own(b, 0) + near(0, b, 1) + near(2 + b, 1 - b, 0),
                own(b, 1) + near(1, b, 0) + near(2 + b, 1 - b, 1),
                near(1, b, 1),
            ], axis=0)
            if b:
                part_out[it, pl.ds(0, 32), :] = line
            else:
                part_own[it] = line
        part_out[it, pl.ds(32, 16), :] = jnp.concatenate([near(2, 0, 0), near(2, 0, 1)], axis=0)
        part_out[it, pl.ds(48, 16), :] = jnp.concatenate([near(3, 1, 0), near(3, 1, 1)], axis=0)
        for j, (start, size, dy) in enumerate(((0, 32, 1), (32, 16, -1), (48, 16, 2))):
            part = pl.ds(start, size)
            sent.append(send(part_out.at[it, part], part_in.at[it, part], part_send.at[it, j],
                             part_recv.at[it, j], at(0, dy)))

    def pass_loads(it):
        for j, (start, size) in enumerate(((0, 32), (32, 16), (48, 16))):
            part = part_in.at[it, pl.ds(start, size)]
            pltpu.make_async_copy(part, part, part_recv.at[it, j]).wait()
        line = part_own[it] + part_in[it, pl.ds(0, 32), :]
        inner = part_in[it, pl.ds(32, 16), :] + part_in[it, pl.ds(48, 16), :]
        edge = jnp.zeros((8, cases), F32)
        load_x[it, ix] = line + jnp.concatenate([edge, inner, edge], axis=0)
        to_line(load_x.at[it, ix], load_x.at[it, ix], load_send.at[it], load_recv.at[it],
                peers_x)

    def share_loads(it):
        wait_all(load_x.at[it], load_recv.at[it])
        for x in range(nx):
            total = load_x[it, (x + 1) % nx, pl.ds(0, 8), :]
            for a in range(3):
                total = total + load_x[it, (x - a) % nx, pl.ds(8 * a + 8, 8), :]
            load_y[it, iy, pl.ds(8 * x, 8), :] = total
        to_line(load_y.at[it, iy], load_y.at[it, iy], load_send.at[ITERS + it],
                load_recv.at[ITERS + it], peers_y)

    block = min(256, slots)
    blocks = slots // block

    def each_block(act):
        if blocks == 1:
            act(0)
            return

        def step(g, carry):
            act(pl.multiple_of(g * block, block))
            return carry

        lax.fori_loop(0, blocks, step, 0)

    def prepare_coarse():
        wait_all(cinv_in, all_recv.at[1])
        per_y = nx * 8
        group = block // per_y

        def order_columns(part, start):
            first = start if isinstance(start, int) else lax.div(start, per_y)
            raw = cinv_in[pl.ds(first, group)].reshape(block, wide)[:, 0:coarse]
            dofs = cinv_in[...].reshape(slots, wide)[:, coarse : coarse + 1]
            spot = lax.broadcasted_iota(jnp.int32, (slots, coarse), 1).astype(F32)
            pick = jnp.where(spot == dofs, 1.0, 0.0).astype(BF16)
            middle[pl.ds(start, block), :] = lax.dot_general(
                split(raw, 2)[part], pick, (((1,), (1,)), ((), ())), preferred_element_type=F32
            ).astype(BF16)

        def order_rows(part, start):
            first = start if isinstance(start, int) else lax.div(start, per_y)
            dofs = cinv_in[pl.ds(first, group)].reshape(block, wide)[:, coarse : coarse + 1]
            spot = lax.broadcasted_iota(jnp.int32, (block, slots), 1)
            device = lax.div(spot, 8)
            inner = lax.rem(spot, 8)
            device = lax.rem(device, nx) * ny + lax.div(device, nx)
            held = jnp.where(inner < 6, 6 * device + inner, -2).astype(F32)
            pick = jnp.where(held == dofs, 1.0, 0.0).astype(BF16)
            inverse[part, pl.ds(start, block), :] = jnp.dot(
                pick, middle[...], preferred_element_type=F32
            ).astype(BF16)

        for part in range(2):
            each_block(functools.partial(order_columns, part))
            each_block(functools.partial(order_rows, part))
        spread_t[...] = spread[:, pl.ds(0, jumps)].astype(F32).T.astype(BF16)

    def solve(it, ratio):
        wait_all(load_y.at[it], load_recv.at[ITERS + it])
        load = load_y[it].reshape(slots, cases)
        if it:
            load = load + ratio * loads_v[it - 1]
        loads_v[it] = load
        both = jnp.concatenate(split(load, 2), axis=1)

        def act(start):
            total = jnp.zeros((block, cases), F32)
            for part in (1, 0):
                product = jnp.dot(inverse[part, pl.ds(start, block), :], both,
                                  preferred_element_type=F32)
                total = total + product[:, cases:]
                total = total + product[:, 0:cases]
            first = start if isinstance(start, int) else lax.div(start, nx * 8)
            solved[pl.ds(first, block // (nx * 8))] = total.reshape(
                block // (nx * 8), nx, 8, cases)

        each_block(act)
        points = {}

        def point(dx, dy):
            if (dx, dy) not in points:
                x, y = at(dx, dy)
                points[dx, dy] = solved[y, x]
            return points[dx, dy]

        pieces = []
        for dx, dy in ((0, 0), (-1, 0), (1, 0), (0, -1), (0, 1)):
            pieces += [point(dx + a, dy + b) for b in range(2) for a in range(2)]
        lift[...] = narrow_dot(spread_t[...], jnp.concatenate(pieces, axis=0), 2)
        return jnp.sum(load * solved[...].reshape(slots, cases), axis=0, keepdims=True)

    precondition(0, 0, first)
    energy = start_energy = None
    ratio = None
    alphas = []
    for it in range(ITERS):
        k = 2 * it
        if it == 0:
            wait_all(cinv_in.at[iy], all_recv.at[0])
            to_line(cinv_in.at[iy], cinv_in.at[iy], all_send.at[1], all_recv.at[1], peers_y)
            loads[6].wait()
            reorder(stiff)
        pass_loads(it)
        if it:
            following = finish_sum(2 * it)
            ratio = following / energy
            energy = following
        for a in (1, 0):
            wait_faces(k, (2 * a, 2 * a + 1))
            for f in (2 * a, 2 * a + 1):
                moved = 0.5 * (image[k, rows[f], :] - got[k, f])
                if it:
                    moved = moved + ratio * way[it - 1, rows[f], :]
                way[it, rows[f], :] = moved
            if a and k + 1 in SPLIT:
                multiply_y(stiff, way[it], k + 1, used)
        walk = way[it]
        act = multiply_x if k + 1 in SPLIT else multiply
        act(stiff, walk, k + 1, pl.ds(0, cut))
        send_x(k + 1, 0, ahead)
        act(stiff, walk, k + 1, pl.ds(cut, cut))
        start_sum(walk[0:jumps] * image[k + 1, used, :], 2 * it + 1)
        send_x(k + 1, ahead, faces - ahead)
        send_faces(k + 1, (2, 3))
        multiply(stiff, walk, k + 1, masked)
        share_loads(it)
        if it == 0:
            prepare_coarse()
            energy = start_energy = finish_sum(0)
        coarse_part = solve(it, ratio)
        alpha = energy / (finish_sum(2 * it + 1) + coarse_part)
        alphas.append(alpha)

        def moved_on(a, k=k + 1, alpha=alpha):
            wait_faces(k, (2 * a, 2 * a + 1))
            for f in (2 * a, 2 * a + 1):
                jump = (image[k, rows[f], :] - got[k, f]) + lift[rows[f], :]
                field[rows[f], :] = field[rows[f], :] - alpha * jump

        precondition(k + 2, 2 * it + 2, moved_on)

    for a in range(2):
        total = alphas[0] * way[0, rows[2 * a + 1], :]
        for it in range(1, ITERS):
            total = total + alphas[it] * way[it, rows[2 * a + 1], :]
        mult_v[a] = total
    mult_v[2] = jnp.zeros(mult_v.shape[1:], F32)
    result = pltpu.make_async_copy(mult_v, mult_hbm, local_sem.at[7])
    result.start()

    for copy in setup + sent:
        copy.wait_send()
    wait_all(cinv_in.at[iy], all_send.at[0])
    wait_all(cinv_in, all_send.at[1])
    for it in range(ITERS):
        wait_all(load_x.at[it], load_send.at[it])
        wait_all(load_y.at[it], load_send.at[ITERS + it])
    for k in range(SUMS - 1):
        wait_all(sums_in.at[k], sum_send.at[k])
    result.wait()
    reduction_ref[...] = finish_sum(SUMS - 1) / start_energy
    wait_all(sums_in.at[SUMS - 1], sum_send.at[SUMS - 1])


def finish(mult_ref, reduction_ref, mult_out, reduction_out):
    mult_out[...] = mult_ref[...]
    reduction_out[...] = reduction_ref[...]


def local(nx, ny, rhs, stiff_inverse, schur, phi, coarse_inverse, incidence, pairing):
    n = nx * ny
    faces, cases = rhs.shape[4], rhs.shape[5]
    interface = stiff_inverse.shape[3]
    corners = phi.shape[3]
    coarse = coarse_inverse.shape[1]
    nodes = incidence.shape[3]
    slots = 8 * n
    span = -(-faces // 128) * 128
    wide = (coarse // 128 + 1) * 128
    reach = max(sum(window(f, faces)[::2]) for f in range(4))
    vmem = pl.BlockSpec(memory_space=pltpu.VMEM)
    anywhere = pl.BlockSpec(memory_space=pl.ANY)
    dma = pltpu.SemaphoreType.DMA
    shapes = (
        jax.ShapeDtypeStruct((3, faces, cases), F32),
        jax.ShapeDtypeStruct((1, cases), F32),
    )
    results = pl.pallas_call(
        functools.partial(kernel, nx, ny),
        out_shape=shapes,
        in_specs=[anywhere] * 7,
        out_specs=(anywhere, vmem),
        scratch_shapes=[
            pltpu.VMEM((3, faces, cases), F32),
            pltpu.VMEM((interface, interface), BF16),
            pltpu.VMEM((interface, interface), BF16),
            pltpu.VMEM((corners, interface), BF16),
            pltpu.VMEM(coarse_inverse.shape, F32),
            pltpu.VMEM((1, nodes), jnp.int32),
            pltpu.VMEM((3, 1, faces), jnp.int32),
            pltpu.VMEM((4, corners, span), F32),
            pltpu.VMEM((160, reach), BF16),
            pltpu.VMEM((4 * faces, 160), BF16),
            pltpu.VMEM((4, corners, span), F32),
            pltpu.VMEM((2, faces, cases), F32),
            pltpu.VMEM((2, 1, faces), jnp.int32),
            pltpu.VMEM((EXCHANGES, 4, faces, cases), F32),
            pltpu.VMEM((interface, cases), F32),
            pltpu.VMEM((ITERS, interface, cases), F32),
            pltpu.VMEM((EXCHANGES + 1, interface, cases), F32),
            pltpu.VMEM((SUMS, 1, cases), F32),
            pltpu.VMEM((SUMS, n, 1, cases), F32),
            pltpu.VMEM((8, wide), F32),
            pltpu.VMEM((ny, nx, 8, wide), F32),
            pltpu.VMEM((slots, slots), BF16),
            pltpu.VMEM((2, slots, slots), BF16),
            pltpu.VMEM((ITERS, 64, cases), F32),
            pltpu.VMEM((ITERS, 64, cases), F32),
            pltpu.VMEM((ITERS, 32, cases), F32),
            pltpu.VMEM((ITERS, nx, 32, cases), F32),
            pltpu.VMEM((ITERS, ny, nx * 8, cases), F32),
            pltpu.VMEM((ITERS, slots, cases), F32),
            pltpu.VMEM((ny, nx, 8, cases), F32),
            pltpu.VMEM((4 * faces, cases), F32),
            pltpu.VMEM((3, faces, cases), F32),
            dma((8,)),
            dma((8,)),
            dma((8,)),
            dma((EXCHANGES, 4)),
            dma((EXCHANGES, 4)),
            dma((SUMS,)),
            dma((SUMS,)),
            dma((2,)),
            dma((2,)),
            dma((ITERS, 3)),
            dma((ITERS, 3)),
            dma((2 * ITERS,)),
            dma((2 * ITERS,)),
        ],
        compiler_params=pltpu.CompilerParams(
            collective_id=0, has_side_effects=True, vmem_limit_bytes=67043328
        ),
    )(
        rhs.reshape(3, faces, cases),
        stiff_inverse.reshape(interface, interface),
        schur.reshape(interface, interface),
        phi.reshape(corners, interface),
        coarse_inverse,
        incidence.reshape(1, nodes),
        pairing.reshape(3, 1, faces),
    )
    multipliers, reduction = pl.pallas_call(
        finish, out_shape=shapes, in_specs=[vmem] * 2, out_specs=(vmem, vmem)
    )(*results)
    return multipliers.reshape(rhs.shape), reduction.reshape(cases)


def solution(mesh):
    nx, ny = mesh.shape["gx"], mesh.shape["gy"]
    return jax.shard_map(
        functools.partial(local, nx, ny),
        mesh=mesh,
        in_specs=(
            P("gx", "gy", None, None, None, None),
            P("gx", "gy", None, None, None),
            P("gx", "gy", None, None, None),
            P("gx", "gy", None, None, None),
            P(("gx", "gy"), None),
            P("gx", "gy", None, None),
            P("gx", "gy", None, None, None),
        ),
        out_specs=(P("gx", "gy", None, None, None, None), P()),
        check_vma=False,
    )
```

```python
import functools

import jax
import jax.numpy as jnp
from jax import lax
from jax.experimental import pallas as pl
from jax.experimental.pallas import tpu as pltpu
from jax.sharding import PartitionSpec as P

ITERS = 2
EXCHANGES = 2 * ITERS
SUMS = 2 * ITERS + 1
SPLIT = (0, *range(1, EXCHANGES, 2))
MESH = pl.DeviceIdType.MESH
F32 = jnp.float32
BF16 = jnp.bfloat16


def split(value, parts):
    pieces = []
    for _ in range(parts):
        piece = value.astype(BF16)
        pieces.append(piece)
        value = value - piece.astype(F32)
    return pieces


def narrow_dot(matrix, value, parts):
    width = value.shape[1]
    product = jnp.dot(
        matrix, jnp.concatenate(split(value, parts), axis=1), preferred_element_type=F32
    )
    total = product[:, (parts - 1) * width :]
    for part in range(parts - 2, -1, -1):
        total = total + product[:, part * width : (part + 1) * width]
    return total


def window(face, faces):
    start = face * faces // 128 * 128
    offset = face * faces - start
    return start, offset, -(-(offset + faces) // 128) * 128


def square_window(face, faces):
    start = face * faces // 128 * 128
    offset = face * faces - start
    return start, offset, -(-(offset + faces) // 256) * 256


def kernel(
    nx, ny, rhs_hbm, stiff_hbm, schur_hbm, phi_hbm, cinv_hbm, inc_hbm, pair_hbm,
    mult_hbm, reduction_ref,
    rhs_v, stiff, schur, phi_ref, cinv_ref, inc_ref, pair_ref, phi_f, spread, spread_t, near_phi, got_rhs, got_pair, got,
    field, way, image, sums_out, sums_in, cinv_out, cinv_in, middle, inverse,
    part_out, part_in, part_own, load_x, load_y, loads_v, solved, lift, mult_v,
    local_sem, setup_send, setup_recv, face_send, face_recv, sum_send, sum_recv,
    all_send, all_recv, part_send, part_recv, load_send, load_recv,
):
    n = nx * ny
    faces = rhs_v.shape[1]
    interface = stiff.shape[0]
    cases = rhs_v.shape[2]
    jumps = 4 * faces
    coarse = cinv_hbm.shape[1]
    slots = n * 8
    span = phi_f.shape[2]
    ix, iy = lax.axis_index("gx"), lax.axis_index("gy")
    me = ix * ny + iy

    def at(dx, dy):
        return lax.rem(ix + (dx + nx), nx), lax.rem(iy + (dy + ny), ny)

    across = [at(-1, 0), at(1, 0), at(0, -1), at(0, 1)]
    rows = [pl.ds(f * faces, faces) for f in range(6)]

    sources = [rhs_hbm, pair_hbm, phi_hbm, inc_hbm, cinv_hbm, schur_hbm, stiff_hbm]
    targets = [rhs_v, pair_ref, phi_ref, inc_ref, cinv_ref, schur, stiff]
    loads = [
        pltpu.make_async_copy(source, target, local_sem.at[i])
        for i, (source, target) in enumerate(zip(sources, targets))
    ]

    ways_x = [at(d, 0)[0] for d in range(nx)]
    ways_y = [at(0, d)[1] for d in range(ny)]
    peers_x = [(x, iy) for x in ways_x[1:]]
    peers_y = [(ix, y) for y in ways_y[1:]]

    def each_peer(act):
        if n <= 64:
            for x in range(nx):
                for y in range(ny):
                    if x or y:
                        act((ways_x[x], ways_y[y]))
            return

        def step(k, carry):
            other = lax.rem(me + k, n)
            act((lax.div(other, ny), lax.rem(other, ny)))
            return carry

        lax.fori_loop(1, n, step, 0)

    for copy in loads[:5]:
        copy.start()
    barrier = pltpu.get_barrier_semaphore()
    each_peer(lambda target: pl.semaphore_signal(
        barrier, inc=1, device_id=target, device_id_type=MESH))

    for copy in loads[5:]:
        copy.start()

    corners = phi_ref.shape[0]
    row = lax.broadcasted_iota(jnp.int32, (32, corners), 0)
    col = lax.broadcasted_iota(jnp.int32, (32, corners), 1)
    point, inner = lax.div(row, 8), lax.rem(row, 8)
    source = 3 * (point + 4 * lax.div(inner, 3)) + lax.rem(inner, 3)
    order = jnp.where((col == source) & (inner < 6), 1.0, 0.0).astype(BF16)
    for i in range(1, 5):
        loads[i].wait()
    reach = spread.shape[1]
    whole_phi = phi_ref[:, pl.ds(0, reach)]
    spread[pl.ds(0, 32), :] = jnp.dot(
        order, whole_phi, preferred_element_type=F32
    ).astype(BF16)
    for f in range(4):
        start, offset, width = window(f, faces)
        piece = phi_ref[:, pl.ds(start, width)].astype(F32)
        if offset:
            piece = pltpu.roll(piece, width - offset, axis=1)
        phi_f[f] = piece[:, 0:span]
    row = lax.broadcasted_iota(jnp.int32, (8, 8), 0)
    col = lax.broadcasted_iota(jnp.int32, (8, 8), 1)
    ids = jnp.broadcast_to(inc_ref[...].astype(F32), (8, 8))
    ids = jnp.sum(jnp.where(col == 4 * lax.div(row, 3), ids, 0.0), axis=1, keepdims=True)
    wide = cinv_out.shape[1]
    row = lax.broadcasted_iota(jnp.int32, (8, wide), 0)
    ids = 3.0 * jnp.broadcast_to(ids, (8, wide)) + lax.rem(row, 3).astype(F32)
    ids = jnp.where(row < 6, ids, -1.0)
    own = jnp.concatenate([cinv_ref[...], jnp.zeros((2, coarse), F32)], axis=0)
    own = jnp.concatenate([own, jnp.zeros((8, wide - coarse), F32)], axis=1)
    lanes = lax.broadcasted_iota(jnp.int32, (8, wide), 1)
    own = jnp.where(lanes == coarse, ids, own)
    cinv_out[...] = own
    cinv_in[iy, ix] = own

    loads[0].wait()
    pl.semaphore_wait(barrier, n - 1)

    def send(src, dst, send_sem, recv_sem, target):
        copy = pltpu.make_async_remote_copy(
            src_ref=src, dst_ref=dst, send_sem=send_sem, recv_sem=recv_sem,
            device_id=target, device_id_type=MESH,
        )
        copy.start()
        return copy

    def to_all(src, slots, send_sem, recv_sem):
        each_peer(lambda target: send(src, slots.at[me], send_sem, recv_sem, target))

    def to_line(src, dst, send_sem, recv_sem, targets):
        for target in targets:
            send(src, dst, send_sem, recv_sem, target)

    def wait_all(slots, sem):
        whole = slots.at[pl.ds(0, slots.shape[0] - 1)]
        pltpu.make_async_copy(whole, whole, sem).wait()

    setup = []
    for a in range(2):
        setup.append(send(pair_ref.at[a], got_pair.at[a], setup_send.at[a], setup_recv.at[a],
                          across[2 * a + 1]))
    for a in range(2):
        setup.append(send(rhs_v.at[a], got_rhs.at[a], setup_send.at[2 + a],
                          setup_recv.at[2 + a], across[2 * a + 1]))
    for f in range(4):
        setup.append(send(phi_f.at[f], near_phi.at[f ^ 1], setup_send.at[4 + f],
                          setup_recv.at[4 + (f ^ 1)], across[f]))
    to_line(cinv_out, cinv_in.at[iy, ix], all_send.at[0], all_recv.at[0], peers_x)

    def turned(pair_row, offset, width):
        lanes = lax.broadcasted_iota(jnp.int32, (1, width), 1)
        if width > faces:
            pair_row = jnp.concatenate(
                [pair_row, jnp.zeros((1, width - faces), jnp.int32)], axis=1
            )
        if offset:
            pair_row = pltpu.roll(pair_row, offset, axis=1)
        inside = (lanes >= offset) & (lanes < offset + faces)
        target = jnp.where(inside, pair_row + offset, lanes)
        place = lax.broadcasted_iota(jnp.int32, (width, width), 0)
        return jnp.where(place == target, 1.0, 0.0)

    turns = []
    for a in range(2):
        setup[a].wait_recv()
        start, offset, width = square_window(2 * a, faces)
        by_col = turned(got_pair[a], offset, width)
        turns.append((start, width, by_col.T.astype(BF16), by_col.astype(BF16)))

    def reorder(matrix):
        for start, width, by_row, _ in turns:
            band = matrix[pl.ds(start, width), :]
            matrix[pl.ds(start, width), :] = jnp.dot(
                by_row, band, preferred_element_type=F32
            ).astype(BF16)
        for start, width, _, by_col in turns:
            band = matrix[:, pl.ds(start, width)]
            matrix[:, pl.ds(start, width)] = jnp.dot(
                band, by_col, preferred_element_type=F32
            ).astype(BF16)

    loads[5].wait()
    reorder(schur)

    for start, width, _, by_col in turns:
        spread[pl.ds(0, 32), pl.ds(start, width)] = jnp.dot(
            spread[pl.ds(0, 32), pl.ds(start, width)], by_col, preferred_element_type=F32
        ).astype(BF16)
    spread[pl.ds(32, 128), :] = jnp.zeros((128, spread.shape[1]), BF16)

    cut = 2 * faces
    ahead = faces // 32 * 8
    low_cut, high_cut = cut // 128 * 128, -(-cut // 128) * 128

    def multiply_y(matrix, value, k, part):
        low = value[cut:].astype(BF16)
        if cut > low_cut:
            low = jnp.concatenate([jnp.zeros((cut - low_cut, cases), BF16), low], axis=0)
        image[k, part, :] = jnp.dot(matrix[part, pl.ds(low_cut, interface - low_cut)], low,
                                    preferred_element_type=F32)

    def multiply_x(matrix, value, k, part):
        low = value[0:cut].astype(BF16)
        if high_cut > cut:
            low = jnp.concatenate([low, jnp.zeros((high_cut - cut, cases), BF16)], axis=0)
        image[k, part, :] = image[k, part, :] + jnp.dot(
            matrix[part, pl.ds(0, high_cut)], low, preferred_element_type=F32)

    def multiply(matrix, value, k, part):
        image[k, part, :] = jnp.dot(matrix[part, :], value.astype(BF16),
                                    preferred_element_type=F32)

    last_x = jnp.where(ix == nx - 1, 1, 0)

    def send_x(k, start, size):
        for f in (last_x, 1 - last_x):
            part = pl.ds(pl.multiple_of(f * faces + start, 8), size)
            target = lax.rem(ix + 2 * f - 1 + nx, nx)
            sent.append(send(image.at[k, part], got.at[k, 1 - f, pl.ds(start, size)],
                             face_send.at[k, f], face_recv.at[k, 1 - f], (target, iy)))

    def send_faces(k, pair):
        for f in pair:
            sent.append(send(image.at[k, rows[f]], got.at[k, f ^ 1], face_send.at[k, f],
                             face_recv.at[k, f ^ 1], across[f]))

    used, masked = pl.ds(0, jumps), pl.ds(jumps, interface - jumps)

    def start_sum(partial, k):
        total = jnp.sum(partial, axis=0, keepdims=True)
        sums_out[k] = total
        sums_in[k, me] = total
        to_all(sums_out.at[k], sums_in.at[k], sum_send.at[k], sum_recv.at[k])

    def finish_sum(k):
        wait_all(sums_in.at[k], sum_recv.at[k])
        return jnp.sum(sums_in[k], axis=0)

    def wait_faces(k, pair):
        for f in pair:
            pltpu.make_async_copy(got.at[k, f], got.at[k, f], face_recv.at[k, f]).wait()

    zeros = jnp.zeros((2 * faces, cases), F32)
    field[pl.ds(jumps, 2 * faces), :] = zeros
    for k in range(ITERS):
        way[k, pl.ds(jumps, 2 * faces), :] = zeros
    sent = []

    def precondition(k, s, ready):
        ready(1)
        if k in SPLIT:
            multiply_y(schur, 0.5 * field[...], k, used)
        ready(0)
        half = 0.5 * field[...]
        act = multiply_x if k in SPLIT else multiply
        act(schur, half, k, pl.ds(0, cut))
        if k == 0:
            send_x(k, 0, faces)
        elif k < EXCHANGES:
            send_x(k, 0, ahead)
        act(schur, half, k, pl.ds(cut, cut))
        if k:
            start_sum(half[0:jumps] * image[k, used, :], s)
        if k == EXCHANGES:
            return
        if k == 0:
            couple()
        else:
            send_x(k, ahead, faces - ahead)
        start_loads(k, k // 2)
        send_faces(k, (2, 3))
        if k == 0:
            start_sum(half[0:jumps] * image[k, used, :], s)
        multiply(schur, half, k, masked)

    def first(a):
        setup[2 + a].wait_recv()
        field[rows[2 * a], :] = -got_rhs[a]
        field[rows[2 * a + 1], :] = rhs_v[a]

    def couple():
        near = []
        for f in range(4):
            setup[4 + (f ^ 1)].wait_recv()
            other = near_phi[f].astype(BF16)
            if f % 2:
                by_col = turned(pair_ref[f // 2], 0, span).astype(BF16)
                other = jnp.dot(other, by_col, preferred_element_type=F32).astype(BF16)
            near.append(other)
        near = jnp.dot(order, jnp.concatenate(near, axis=1), preferred_element_type=F32)
        for f in range(4):
            start, offset, width = window(f, faces)
            other = near[:, f * span : (f + 1) * span]
            if span < width:
                other = jnp.concatenate([other, jnp.zeros((32, width - span), F32)], axis=1)
            if offset:
                other = pltpu.roll(other, offset, axis=1)
            lanes = lax.broadcasted_iota(jnp.int32, (32, width), 1)
            inside = (lanes >= offset) & (lanes < offset + faces)
            other = jnp.where(inside, -other, 0.0)
            spread[pl.ds(32 + 32 * f, 32), pl.ds(start, width)] = other.astype(BF16)

    def start_loads(k, it):
        value = narrow_dot(spread[:, pl.ds(0, jumps)], image[k, pl.ds(0, jumps), :], 2)

        def own(b, a):
            return 0.5 * value[8 * (2 * b + a) : 8 * (2 * b + a) + 8]

        def near(f, b, a):
            return 0.5 * value[32 + 32 * f + 8 * (2 * b + a) : 40 + 32 * f + 8 * (2 * b + a)]

        for b in range(2):
            line = jnp.concatenate([
                near(0, b, 0),
                own(b, 0) + near(0, b, 1) + near(2 + b, 1 - b, 0),
                own(b, 1) + near(1, b, 0) + near(2 + b, 1 - b, 1),
                near(1, b, 1),
            ], axis=0)
            if b:
                part_out[it, pl.ds(0, 32), :] = line
            else:
                part_own[it] = line
        part_out[it, pl.ds(32, 16), :] = jnp.concatenate([near(2, 0, 0), near(2, 0, 1)], axis=0)
        part_out[it, pl.ds(48, 16), :] = jnp.concatenate([near(3, 1, 0), near(3, 1, 1)], axis=0)
        for j, (start, size, dy) in enumerate(((0, 32, 1), (32, 16, -1), (48, 16, 2))):
            part = pl.ds(start, size)
            sent.append(send(part_out.at[it, part], part_in.at[it, part], part_send.at[it, j],
                             part_recv.at[it, j], at(0, dy)))

    def pass_loads(it):
        for j, (start, size) in enumerate(((0, 32), (32, 16), (48, 16))):
            part = part_in.at[it, pl.ds(start, size)]
            pltpu.make_async_copy(part, part, part_recv.at[it, j]).wait()
        line = part_own[it] + part_in[it, pl.ds(0, 32), :]
        inner = part_in[it, pl.ds(32, 16), :] + part_in[it, pl.ds(48, 16), :]
        edge = jnp.zeros((8, cases), F32)
        total = line + jnp.concatenate([edge, inner, edge], axis=0)
        load_x[it, ix] = jnp.concatenate([total[8 * a : 8 * a + 6] for a in range(4)], axis=0)
        to_line(load_x.at[it, ix], load_x.at[it, ix], load_send.at[it], load_recv.at[it],
                peers_x)

    def share_loads(it):
        wait_all(load_x.at[it], load_recv.at[it])
        lines = [load_x[it, x] for x in range(nx)]
        for x in range(nx):
            total = lines[(x + 1) % nx][0:6]
            for a in range(3):
                total = total + lines[(x - a) % nx][6 * a + 6 : 6 * a + 12]
            load_y[it, iy, pl.ds(8 * x, 8), :] = jnp.concatenate(
                [total, jnp.zeros((2, cases), F32)], axis=0)
        to_line(load_y.at[it, iy], load_y.at[it, iy], load_send.at[ITERS + it],
                load_recv.at[ITERS + it], peers_y)

    block = min(256, slots)
    blocks = slots // block

    def each_block(act):
        if blocks == 1:
            act(0)
            return

        def step(g, carry):
            act(pl.multiple_of(g * block, block))
            return carry

        lax.fori_loop(0, blocks, step, 0)

    def prepare_coarse():
        wait_all(cinv_in, all_recv.at[1])
        per_y = nx * 8
        group = block // per_y

        def order_columns(part, start):
            first = start if isinstance(start, int) else lax.div(start, per_y)
            raw = cinv_in[pl.ds(first, group)].reshape(block, wide)[:, 0:coarse]
            dofs = cinv_in[...].reshape(slots, wide)[:, coarse : coarse + 1]
            spot = lax.broadcasted_iota(jnp.int32, (slots, coarse), 1).astype(F32)
            pick = jnp.where(spot == dofs, 1.0, 0.0).astype(BF16)
            middle[pl.ds(start, block), :] = lax.dot_general(
                split(raw, 2)[part], pick, (((1,), (1,)), ((), ())), preferred_element_type=F32
            ).astype(BF16)

        def order_rows(part, start):
            first = start if isinstance(start, int) else lax.div(start, per_y)
            dofs = cinv_in[pl.ds(first, group)].reshape(block, wide)[:, coarse : coarse + 1]
            spot = lax.broadcasted_iota(jnp.int32, (block, slots), 1)
            device = lax.div(spot, 8)
            inner = lax.rem(spot, 8)
            device = lax.rem(device, nx) * ny + lax.div(device, nx)
            held = jnp.where(inner < 6, 6 * device + inner, -2).astype(F32)
            pick = jnp.where(held == dofs, 1.0, 0.0).astype(BF16)
            inverse[part, pl.ds(start, block), :] = jnp.dot(
                pick, middle[...], preferred_element_type=F32
            ).astype(BF16)

        for part in range(2):
            each_block(functools.partial(order_columns, part))
            each_block(functools.partial(order_rows, part))
        spread_t[...] = spread[:, pl.ds(0, jumps)].astype(F32).T.astype(BF16)

    def solve(it, ratio):
        wait_all(load_y.at[it], load_recv.at[ITERS + it])
        load = load_y[it].reshape(slots, cases)
        if it:
            load = load + ratio * loads_v[it - 1]
        loads_v[it] = load
        both = jnp.concatenate(split(load, 2), axis=1)

        def act(start):
            total = jnp.zeros((block, cases), F32)
            for part in (1, 0):
                product = jnp.dot(inverse[part, pl.ds(start, block), :], both,
                                  preferred_element_type=F32)
                total = total + product[:, cases:]
                total = total + product[:, 0:cases]
            first = start if isinstance(start, int) else lax.div(start, nx * 8)
            solved[pl.ds(first, block // (nx * 8))] = total.reshape(
                block // (nx * 8), nx, 8, cases)

        each_block(act)
        points = {}

        def point(dx, dy):
            if (dx, dy) not in points:
                x, y = at(dx, dy)
                points[dx, dy] = solved[y, x]
            return points[dx, dy]

        pieces = []
        for dx, dy in ((0, 0), (-1, 0), (1, 0), (0, -1), (0, 1)):
            pieces += [point(dx + a, dy + b) for b in range(2) for a in range(2)]
        lift[...] = narrow_dot(spread_t[...], jnp.concatenate(pieces, axis=0), 2)
        return jnp.sum(load * solved[...].reshape(slots, cases), axis=0, keepdims=True)

    precondition(0, 0, first)
    energy = start_energy = None
    ratio = None
    alphas = []
    for it in range(ITERS):
        k = 2 * it
        if it == 0:
            wait_all(cinv_in.at[iy], all_recv.at[0])
            to_line(cinv_in.at[iy], cinv_in.at[iy], all_send.at[1], all_recv.at[1], peers_y)
            loads[6].wait()
            reorder(stiff)
        pass_loads(it)
        if it:
            following = finish_sum(2 * it)
            ratio = following / energy
            energy = following
        for a in (1, 0):
            wait_faces(k, (2 * a, 2 * a + 1))
            for f in (2 * a, 2 * a + 1):
                moved = 0.5 * (image[k, rows[f], :] - got[k, f])
                if it:
                    moved = moved + ratio * way[it - 1, rows[f], :]
                way[it, rows[f], :] = moved
            if a and k + 1 in SPLIT:
                multiply_y(stiff, way[it], k + 1, used)
        walk = way[it]
        act = multiply_x if k + 1 in SPLIT else multiply
        act(stiff, walk, k + 1, pl.ds(0, cut))
        send_x(k + 1, 0, ahead)
        act(stiff, walk, k + 1, pl.ds(cut, cut))
        start_sum(walk[0:jumps] * image[k + 1, used, :], 2 * it + 1)
        send_x(k + 1, ahead, faces - ahead)
        send_faces(k + 1, (2, 3))
        multiply(stiff, walk, k + 1, masked)
        share_loads(it)
        if it == 0:
            prepare_coarse()
            energy = start_energy = finish_sum(0)
        coarse_part = solve(it, ratio)
        alpha = energy / (finish_sum(2 * it + 1) + coarse_part)
        alphas.append(alpha)

        def moved_on(a, k=k + 1, alpha=alpha):
            wait_faces(k, (2 * a, 2 * a + 1))
            for f in (2 * a, 2 * a + 1):
                jump = (image[k, rows[f], :] - got[k, f]) + lift[rows[f], :]
                field[rows[f], :] = field[rows[f], :] - alpha * jump

        precondition(k + 2, 2 * it + 2, moved_on)

    for a in range(2):
        total = alphas[0] * way[0, rows[2 * a + 1], :]
        for it in range(1, ITERS):
            total = total + alphas[it] * way[it, rows[2 * a + 1], :]
        mult_v[a] = total
    mult_v[2] = jnp.zeros(mult_v.shape[1:], F32)
    result = pltpu.make_async_copy(mult_v, mult_hbm, local_sem.at[7])
    result.start()

    for copy in setup + sent:
        copy.wait_send()
    wait_all(cinv_in.at[iy], all_send.at[0])
    wait_all(cinv_in, all_send.at[1])
    for it in range(ITERS):
        wait_all(load_x.at[it], load_send.at[it])
        wait_all(load_y.at[it], load_send.at[ITERS + it])
    for k in range(SUMS - 1):
        wait_all(sums_in.at[k], sum_send.at[k])
    result.wait()
    reduction_ref[...] = finish_sum(SUMS - 1) / start_energy
    wait_all(sums_in.at[SUMS - 1], sum_send.at[SUMS - 1])


def finish(mult_ref, reduction_ref, mult_out, reduction_out):
    mult_out[...] = mult_ref[...]
    reduction_out[...] = reduction_ref[...]


def local(nx, ny, rhs, stiff_inverse, schur, phi, coarse_inverse, incidence, pairing):
    n = nx * ny
    faces, cases = rhs.shape[4], rhs.shape[5]
    interface = stiff_inverse.shape[3]
    corners = phi.shape[3]
    coarse = coarse_inverse.shape[1]
    nodes = incidence.shape[3]
    slots = 8 * n
    span = -(-faces // 128) * 128
    wide = (coarse // 128 + 1) * 128
    reach = max(sum(window(f, faces)[::2]) for f in range(4))
    vmem = pl.BlockSpec(memory_space=pltpu.VMEM)
    anywhere = pl.BlockSpec(memory_space=pl.ANY)
    dma = pltpu.SemaphoreType.DMA
    shapes = (
        jax.ShapeDtypeStruct((3, faces, cases), F32),
        jax.ShapeDtypeStruct((1, cases), F32),
    )
    results = pl.pallas_call(
        functools.partial(kernel, nx, ny),
        out_shape=shapes,
        in_specs=[anywhere] * 7,
        out_specs=(anywhere, vmem),
        scratch_shapes=[
            pltpu.VMEM((3, faces, cases), F32),
            pltpu.VMEM((interface, interface), BF16),
            pltpu.VMEM((interface, interface), BF16),
            pltpu.VMEM((corners, interface), BF16),
            pltpu.VMEM(coarse_inverse.shape, F32),
            pltpu.VMEM((1, nodes), jnp.int32),
            pltpu.VMEM((3, 1, faces), jnp.int32),
            pltpu.VMEM((4, corners, span), F32),
            pltpu.VMEM((160, reach), BF16),
            pltpu.VMEM((4 * faces, 160), BF16),
            pltpu.VMEM((4, corners, span), F32),
            pltpu.VMEM((2, faces, cases), F32),
            pltpu.VMEM((2, 1, faces), jnp.int32),
            pltpu.VMEM((EXCHANGES, 4, faces, cases), F32),
            pltpu.VMEM((interface, cases), F32),
            pltpu.VMEM((ITERS, interface, cases), F32),
            pltpu.VMEM((EXCHANGES + 1, interface, cases), F32),
            pltpu.VMEM((SUMS, 1, cases), F32),
            pltpu.VMEM((SUMS, n, 1, cases), F32),
            pltpu.VMEM((8, wide), F32),
            pltpu.VMEM((ny, nx, 8, wide), F32),
            pltpu.VMEM((slots, slots), BF16),
            pltpu.VMEM((2, slots, slots), BF16),
            pltpu.VMEM((ITERS, 64, cases), F32),
            pltpu.VMEM((ITERS, 64, cases), F32),
            pltpu.VMEM((ITERS, 32, cases), F32),
            pltpu.VMEM((ITERS, nx, 24, cases), F32),
            pltpu.VMEM((ITERS, ny, nx * 8, cases), F32),
            pltpu.VMEM((ITERS, slots, cases), F32),
            pltpu.VMEM((ny, nx, 8, cases), F32),
            pltpu.VMEM((4 * faces, cases), F32),
            pltpu.VMEM((3, faces, cases), F32),
            dma((8,)),
            dma((8,)),
            dma((8,)),
            dma((EXCHANGES, 4)),
            dma((EXCHANGES, 4)),
            dma((SUMS,)),
            dma((SUMS,)),
            dma((2,)),
            dma((2,)),
            dma((ITERS, 3)),
            dma((ITERS, 3)),
            dma((2 * ITERS,)),
            dma((2 * ITERS,)),
        ],
        compiler_params=pltpu.CompilerParams(
            collective_id=0, has_side_effects=True, vmem_limit_bytes=67043328
        ),
    )(
        rhs.reshape(3, faces, cases),
        stiff_inverse.reshape(interface, interface),
        schur.reshape(interface, interface),
        phi.reshape(corners, interface),
        coarse_inverse,
        incidence.reshape(1, nodes),
        pairing.reshape(3, 1, faces),
    )
    multipliers, reduction = pl.pallas_call(
        finish, out_shape=shapes, in_specs=[vmem] * 2, out_specs=(vmem, vmem)
    )(*results)
    return multipliers.reshape(rhs.shape), reduction.reshape(cases)


def solution(mesh):
    nx, ny = mesh.shape["gx"], mesh.shape["gy"]
    return jax.shard_map(
        functools.partial(local, nx, ny),
        mesh=mesh,
        in_specs=(
            P("gx", "gy", None, None, None, None),
            P("gx", "gy", None, None, None),
            P("gx", "gy", None, None, None),
            P("gx", "gy", None, None, None),
            P(("gx", "gy"), None),
            P("gx", "gy", None, None),
            P("gx", "gy", None, None, None),
        ),
        out_specs=(P("gx", "gy", None, None, None, None), P()),
        check_vma=False,
    )
```
